128 devices in a mesh: dp: 16 (over z, y), expert: 8 (over x, core).
Axes of the slice: x: 4, y: 4, z: 4, core: 2. Of those that a mesh axis runs over, the one named last changes fastest.
Arguments:
- tokens: bfloat16 [2048, 4096], P('dp'), may hold values from -6 to 6
- expert_ids: int32 [2048, 2], P('dp'), may hold values from 0 to 7, all different within a row; in each aligned block of 128 rows (0 to 127, 128 to 255, ...) at most 96 rows name the same one
- gate_weights: float32 [2048, 2], P('dp'), may hold values from 0.2 to 1
- live_counts: int32 [16], P('dp'), may hold values from 64 to 128, as said below
- w_gate: bfloat16 [8, 4096, 8192], P('expert', None, 'dp'), may hold values from -0.09375 to 0.09375
- w_up: bfloat16 [8, 4096, 8192], P('expert', None, 'dp'), may hold values from -0.09375 to 0.09375
- w_down: bfloat16 [8, 8192, 4096], P('expert', 'dp'), may hold values from -0.0625 to 0.0625
Outputs:
- mixed: bfloat16 [2048, 4096], P('dp')
- total_loads: int32 [8], replicated
The draws below stay inside these ranges and needn't reach their ends.
Inputs may be any that keep to these rules, and one draw needn't show every extreme that they name: `expert_ids`: each token names two different experts. Among the tokens of one rank no expert is named more than 96 times, a bound that some block reaches in some ranks. Rank r's first live_counts[r] tokens are live, the rest are padding. Some rank has all 128 tokens live.
All inputs are finite; a program needn't handle non-finite values.
Results may differ from the reference program's by a relative error of at most 0.017.
Values may be sent and summed in bfloat16 or wider, within the bound.
A program may use at most 128 MiB of HBM per device.

```python
import math
import jax
import jax.numpy as jnp
import numpy as np
from jax import lax

D = 4096
FF = 8192
TOK_DEV = 128
EXPERTS = 8
CAP = 96
RANKS = 16
TOKENS = 2048
N_DP = 16


def draw_live_counts(key, part):
    base = jax.random.fold_in(key, 11)
    first_key, second_key = jax.random.split(base)
    counts = jax.random.randint(first_key, (RANKS,), TOK_DEV // 2, TOK_DEV + 1)
    full_rank = jax.random.randint(second_key, (), 0, RANKS)
    return jnp.where(jnp.arange(RANKS) == full_rank, TOK_DEV, counts).astype(jnp.int32)


def shard_levels(rng, dims, cuts, smallest, high):
    loudness = 1.0
    for axis_at, blocks in cuts:
        draws = jax.random.uniform(jax.random.fold_in(jax.random.fold_in(rng, 6), axis_at), (blocks,), jnp.float32, smallest / len(cuts), high / len(cuts))
        loudness = loudness * jnp.repeat(jnp.exp(draws), dims[axis_at] // blocks).reshape((-1,) + (1,) * (len(dims) - 1 - axis_at))
    return loudness


def shared_out(rng, own, number, rows, count, top, bound, slope):
    ranking = jax.random.permutation(rng, count)
    packed, usual = load_shares(count, rows * top, bound, slope, True), load_shares(count, rows * top, bound, slope, False)
    places = jnp.arange(count)

    def named(sizes, offset_by):
        used = int((sizes > 0).sum())
        fixed = max(1, used // 4)
        passed = fixed + (places - fixed + offset_by * (used - fixed)) % max(1, count - fixed)
        return jnp.zeros((count,), jnp.int32).at[ranking[jnp.where(places < fixed, places, passed)]].set(jnp.asarray(sizes, jnp.int32))

    sizes = jnp.where(number % 4 == 0, named(packed, number // 4), named(usual, number - number // 4 - 1))
    mixed = jax.random.permutation(jax.random.fold_in(own, 3), count)
    donor, receiver = mixed[0:count // 2 * 2:2], mixed[1:count // 2 * 2:2]
    margin = jnp.minimum(sizes[donor] - 1, bound - sizes[receiver]) // 2
    margin = jnp.where((donor == ranking[0]) | (receiver == ranking[0]) | (sizes[receiver] == 0), 0, jnp.maximum(margin, 0))
    passed = jax.random.randint(jax.random.fold_in(own, 4), (count // 2,), 0, 1 << 20) % (margin + 1)
    sizes = sizes.at[donor].add(-passed).at[receiver].add(passed)
    items = jnp.searchsorted(jnp.cumsum(sizes), jnp.arange(rows * top), side="right").astype(jnp.int32)
    grid = items.reshape(top, rows).T
    grid = grid[jax.random.permutation(jax.random.fold_in(own, 1), rows)]
    offset_by = jax.random.randint(jax.random.fold_in(own, 2), (rows, 1), 0, top)
    return jnp.take_along_axis(grid, (jnp.arange(top)[None, :] + offset_by) % top, axis=1)


def load_shares(amount, total, bound, lean, full):
    portions = [(1 << 20) // math.isqrt(standing ** lean) + 1 for standing in range(1, amount + 1)]
    largest = bound if full else min(bound, max(-(-total // amount), total * portions[0] // sum(portions)))
    least = 1 if total - largest >= amount - 1 else 0
    given, spare = [largest] + [least] * (amount - 1), total - largest - least * (amount - 1)
    while spare > 0:
        movable = [i for i in range(1, amount) if given[i] < largest] or [i for i in range(1, amount) if given[i] < bound]
        whole, left = sum([portions[i] for i in movable]), spare
        for i in movable:
            more = min(bound - given[i], max(1, left * portions[i] // whole), spare)
            given[i] = given[i] + more
            spare = spare - more
    return np.array(given)


def gaussian(own_key, extent, width, bound, pieces=(), held_as=jnp.bfloat16):
    result = width * jax.random.normal(own_key, extent, jnp.float32)
    if pieces:
        result = result * shard_levels(own_key, extent, pieces, -0.22, 0.18)
    return jnp.clip(result, -bound, bound).astype(held_as)


def setup_inputs(seed: int = 0) -> dict:
    streams_of = jax.random.split(jax.random.key(seed), 8)
    tokens = gaussian(streams_of[0], (TOKENS, D), 1.0, 6.0, ((0, 16),))
    expert_ids_keys = jax.random.split(jax.random.fold_in(streams_of[1], 1), TOKENS // TOK_DEV)
    expert_ids_turns = jax.random.permutation(jax.random.fold_in(streams_of[1], 3), TOKENS // TOK_DEV)
    expert_ids = jax.vmap(lambda own, number: shared_out(jax.random.fold_in(streams_of[1], 2), own, number, TOK_DEV, EXPERTS, 2, CAP, 2))(expert_ids_keys, expert_ids_turns).reshape((TOKENS, 2))
    gate_weights = jnp.clip(0.2 + 0.8 * jax.random.uniform(streams_of[2], (TOKENS, 2), jnp.float32) ** shard_levels(streams_of[2], (TOKENS, 2), ((0, 16),), -0.2, 0.2), 0.2, 1.0)
    live_counts = draw_live_counts(jax.random.fold_in(streams_of[7], 71), 0)
    w_gate = gaussian(streams_of[4], (EXPERTS, D, FF), D ** -0.5, 0.09375, ((0, 8), (2, 16)))
    w_up = gaussian(streams_of[5], (EXPERTS, D, FF), D ** -0.5, 0.09375, ((0, 8), (2, 16)))
    w_down = gaussian(streams_of[6], (EXPERTS, FF, D), FF ** -0.5, 0.0625, ((0, 8), (1, 16)))
    return {"tokens": tokens, "expert_ids": expert_ids, "gate_weights": gate_weights, "live_counts": live_counts, "w_gate": w_gate, "w_up": w_up, "w_down": w_down}


def plan_routes(expert_ids, live_total, n_experts, capacity):
    row_count = expert_ids.shape[0]
    is_live = jnp.arange(row_count, dtype=jnp.int32) < live_total
    flat_ids = expert_ids.reshape(-1)
    live_pairs = jnp.repeat(is_live, 2)
    one_hot = ((flat_ids[:, None] == jnp.arange(n_experts, dtype=jnp.int32)[None, :]) & live_pairs[:, None]).astype(jnp.int32)
    earlier = jnp.cumsum(one_hot, axis=0) - one_hot
    slot_index = jnp.sum(earlier * one_hot, axis=1)
    targets = jnp.where(live_pairs, flat_ids * capacity + slot_index, -1).astype(jnp.int32)
    return targets.reshape(row_count, 2), jnp.sum(one_hot, axis=0)


def dispatch_rows(tokens, targets, slots_all):
    wanted = targets.reshape(-1)[None, :] == jnp.arange(slots_all, dtype=jnp.int32)[:, None]
    wanted = jnp.any(wanted.reshape(slots_all, -1, 2), axis=2).astype(jnp.bfloat16)
    return jnp.dot(wanted, tokens, preferred_element_type=jnp.float32).astype(jnp.bfloat16)


def combine_rows(results, targets, gate_weights):
    pick_index = jnp.maximum(targets, 0).astype(jnp.int32)
    selected = results[pick_index].astype(jnp.float32)
    weights = jnp.where(targets >= 0, gate_weights, jnp.zeros_like(gate_weights))
    return jnp.sum(weights[:, :, None] * selected, axis=1).astype(jnp.bfloat16)


def reference(tokens, expert_ids, gate_weights, live_counts, w_gate, w_up, w_down):
    tok_blocks = tokens.reshape(RANKS, TOK_DEV, D)
    id_blocks = expert_ids.reshape(RANKS, TOK_DEV, 2)
    gate_blocks = gate_weights.reshape(RANKS, TOK_DEV, 2)
    targets, loads = jax.vmap(lambda ids, live: plan_routes(ids, live, EXPERTS, CAP))(id_blocks, live_counts)
    outbound = jax.vmap(lambda toks, tgt: dispatch_rows(toks, tgt, EXPERTS * CAP))(tok_blocks, targets)
    per_expert = outbound.reshape(RANKS, EXPERTS, CAP, D).transpose(1, 0, 2, 3).reshape(EXPERTS, RANKS * CAP, D)
    shard_width = FF // N_DP

    def run_expert(operands):
        row_block, gate_matrix, up_matrix, down_matrix = operands
        total = jnp.zeros((row_block.shape[0], D), jnp.float32)
        for shard_index in range(N_DP):
            lower = shard_index * shard_width
            gate_act = jnp.dot(row_block, gate_matrix[:, lower:lower + shard_width], preferred_element_type=jnp.float32)
            up_act = jnp.dot(row_block, up_matrix[:, lower:lower + shard_width], preferred_element_type=jnp.float32)
            hidden = (jax.nn.silu(gate_act) * up_act).astype(jnp.bfloat16)
            partial_term = jnp.dot(hidden, down_matrix[lower:lower + shard_width, :], preferred_element_type=jnp.float32).astype(jnp.bfloat16)
            partial_term = lax.optimization_barrier(partial_term)
            total = total + partial_term.astype(jnp.float32)
        return total.astype(jnp.bfloat16)

    results = lax.map(run_expert, (per_expert, w_gate, w_up, w_down))
    returned = results.reshape(EXPERTS, RANKS, CAP, D).transpose(1, 0, 2, 3).reshape(RANKS, EXPERTS * CAP, D)
    mixed = jax.vmap(combine_rows)(returned, targets, gate_blocks).reshape(TOKENS, D)
    return mixed, jnp.sum(loads, axis=0).astype(jnp.int32)
```

```python
import functools
import jax
import jax.numpy as jnp
from jax import lax
from jax.experimental import pallas as pl
from jax.experimental.pallas import tpu as pltpu
from jax.sharding import Mesh
from jax.sharding import PartitionSpec as P

MESH = pl.DeviceIdType.MESH
DP = ("z", "y")
EXPERT = ("x", "c")
RINGS = (("y", "z"), ("z", "y"))
VMEM_LIMIT = 67043328


def shifted(axis, by):
    return lax.rem(lax.axis_index(axis) + by % 4, 4)


def other_core():
    return {"c": 1 - lax.axis_index("c")}


class Sender:
    def __init__(self, sems):
        self.sems, self.copies = sems, []

    def __call__(self, src, dst, recv_sem, where):
        copy = pltpu.make_async_remote_copy(
            src_ref=src,
            dst_ref=dst,
            send_sem=self.sems.at[len(self.copies)],
            recv_sem=recv_sem,
            device_id=where,
            device_id_type=MESH,
        )
        copy.start()
        self.copies.append(copy)

    def drain(self):
        for copy in self.copies:
            copy.wait_send()


def landed(ref, sem):
    pltpu.make_async_copy(ref, ref, sem).wait()


def enter(peers):
    barrier = pltpu.get_barrier_semaphore()
    for peer in peers:
        pl.semaphore_signal(barrier, inc=1, device_id=peer, device_id_type=MESH)
    pl.semaphore_wait(barrier, len(peers))


def gather_kernel(
    tok, meta, wg_hbm, wu_hbm, hid, loads, x, wg, wu, m, wcol, wsem, send_sem, blk_sem, half_sem, swap_sem, meta_sem
):
    c = lax.axis_index("c")
    expert = lax.axis_index("x") * 2 + c
    loads_in = [pltpu.make_async_copy(wg_hbm, wg, wsem.at[0]), pltpu.make_async_copy(wu_hbm, wu, wsem.at[1])]
    for copy in loads_in:
        copy.start()
    rows = x.shape[4]
    half = rows // 2
    peers = [(i, j) for i in range(4) for j in range(4) if (i, j) != (0, 0)]
    enter([other_core()] + [{"z": shifted("z", i), "y": shifted("y", j)} for i, j in peers])
    send = Sender(send_sem)

    def own_rows(h, o):
        owner = c if o == 0 else 1 - c
        return pl.ds(pl.multiple_of(owner * (2 * rows) + h * rows, rows), rows)

    for h in range(2):
        mine = tok.at[own_rows(h, 0)]
        a1, a2 = RINGS[h]
        send(mine, x.at[h, 0, 0, 3], blk_sem.at[h, 0, 3], {a1: shifted(a1, 1)})
        send(mine, x.at[h, 0, 0, 1], blk_sem.at[h, 0, 1], {a1: shifted(a1, -1)})
    for h in range(2):
        mine = tok.at[own_rows(h, 0)]
        a1, a2 = RINGS[h]
        send(mine, x.at[h, 3, 0, 0], blk_sem.at[h, 3, 0], {a2: shifted(a2, 1)})
        send(mine, x.at[h, 1, 0, 0], blk_sem.at[h, 1, 0], {a2: shifted(a2, -1)})
    for i, j in peers:
        at = (-i % 4, -j % 4)
        send(meta, m.at[at], meta_sem.at[at], {"z": shifted("z", i), "y": shifted("y", j)})
    m[0, 0] = meta[...]
    for h in range(2):
        for o in range(2):
            x[h, 0, o, 0] = tok[own_rows(h, o), :]

    def swap(h, g, b):
        send(x.at[h, g, 0, b], x.at[h, g, 1, b], swap_sem.at[h, g, b], other_core())

    def spread(h, b):
        a2 = RINGS[h][1]
        send(x.at[h, 0, 0, b], x.at[h, 3, 0, b], blk_sem.at[h, 3, b], {a2: shifted(a2, 1)})
        send(x.at[h, 0, 0, b], x.at[h, 1, 0, b], blk_sem.at[h, 1, b], {a2: shifted(a2, -1)})
        swap(h, 0, b)

    def near(h):
        a1 = RINGS[h][0]
        for b, step, part in ((3, 1, 0), (1, -1, 1)):
            landed(x.at[h, 0, 0, b], blk_sem.at[h, 0, b])
            piece = pl.ds(part * half, half)
            send(
                x.at[h, 0, 0, b, piece], x.at[h, 0, 0, 2, piece], half_sem.at[h, part], {a1: shifted(a1, step)}
            )
            spread(h, b)

    def far(h):
        for part in range(2):
            landed(x.at[h, 0, 0, 2, pl.ds(part * half, half)], half_sem.at[h, part])
        spread(h, 2)

    def onward(h, b):
        a2 = RINGS[h][1]
        for g, step, passes in ((3, 1, (0, 2)), (1, -1, (3, 1))):
            landed(x.at[h, g, 0, b], blk_sem.at[h, g, b])
            if b in passes:
                send(x.at[h, g, 0, b], x.at[h, 2, 0, b], blk_sem.at[h, 2, b], {a2: shifted(a2, step)})
            swap(h, g, b)

    def last(h, b):
        landed(x.at[h, 2, 0, b], blk_sem.at[h, 2, b])
        swap(h, 2, b)

    def weigh():
        for i, j in peers:
            landed(m.at[i, j], meta_sem.at[i, j])
        total = jnp.zeros(m.shape[2:], jnp.float32)
        for i in range(4):
            for j in range(4):
                total = total + jnp.where(m[i, j] > 0.0, 1.0, 0.0)
                row = m[i, j, pl.ds(expert, 1), :]
                wcol[i, j] = jnp.transpose(jnp.broadcast_to(row, (row.shape[1], row.shape[1])))
        loads[...] = jnp.broadcast_to(jnp.sum(total, axis=1, keepdims=True), loads.shape).astype(jnp.int32)

    def compute(h, g):
        for b in range(4):
            if (g, b) != (0, 0):
                landed(x.at[h, g, 1, b], swap_sem.at[h, g, b])
        parts = []
        for o in range(2):
            for b in range(4):
                at = (g, b) if h == 0 else (b, g)
                parts.append(wcol[at[0], at[1], own_rows(h, o), :])
        weight = jnp.concatenate(parts, axis=0)
        weight = jnp.concatenate([weight, weight], axis=1)

        @pl.loop(0, 2)
        def _(n):
            cols = pl.ds(pl.multiple_of(n * 256, 256), 256)
            lhs = x[h, g].reshape(8 * rows, x.shape[5])
            gate = jnp.dot(lhs, wg[:, cols], preferred_element_type=jnp.float32)
            up = jnp.dot(lhs, wu[:, cols], preferred_element_type=jnp.float32)
            act = gate / (1.0 + jnp.exp(-gate)) * up * weight
            hid[h, g, :, cols] = act.astype(jnp.bfloat16)

    near(0), near(1)
    onward(0, 0), onward(1, 0)
    far(0), far(1)
    weigh()
    for copy in loads_in:
        copy.wait()
    compute(0, 0)
    onward(0, 3), onward(1, 3)
    compute(1, 0)
    onward(0, 1), onward(1, 1)
    last(0, 0), last(1, 0)
    onward(0, 2), onward(1, 2)
    compute(0, 3)
    last(0, 3), last(1, 3)
    compute(0, 1)
    last(0, 1), last(1, 1)
    compute(1, 3)
    compute(1, 1)
    last(0, 2), last(1, 2)
    compute(0, 2)
    compute(1, 2)
    send.drain()


def scatter_kernel(
    hid, wd_hbm, out, wd, s, p, l, f, n1, t, f2, n2, r, xr, ob, wsem, send_sem, l_sem, f_sem, n_sem, f2_sem, n2_sem,
    x_sem, ox_sem, od_sem, out_sem,
):
    c, xi = lax.axis_index("c"), lax.axis_index("x")
    load = pltpu.make_async_copy(wd_hbm, wd, wsem)
    load.start()
    rows, width = s.shape[3], s.shape[4]
    half = rows // 2
    enter(
        [other_core()]
        + [{a: shifted(a, by)} for a in ("y", "z") for by in (1, -1)]
        + [{"x": shifted("x", by)} for by in (1, 2, 3)]
    )
    send = Sender(send_sem)
    load.wait()
    f32 = lambda v: v.astype(jnp.float32)
    bf16 = lambda v: v.astype(jnp.bfloat16)

    def compute(h, g):
        @pl.loop(0, width // 512)
        def _(n):
            cols = pl.ds(pl.multiple_of(n * 512, 512), 512)
            y = bf16(jnp.dot(hid[h, g], wd[:, cols], preferred_element_type=jnp.float32))
            s[h, g, :, :, cols] = y[: 4 * rows].reshape(4, rows, 512)
            p[h, g, :, :, cols] = y[4 * rows :].reshape(4, rows, 512)

        send(p.at[h, g], l.at[h, g], l_sem.at[h, g], other_core())

    def chip_sum(h, g):
        landed(l.at[h, g], l_sem.at[h, g])

        @pl.loop(0, 4)
        def _(b):
            s[h, g, b] = bf16(f32(s[h, g, b]) + f32(l[h, g, b]))

    ways = ((1, 0, (2, 0)), (-1, 1, (1, 3)))

    def send_far(h):
        a2 = RINGS[h][1]
        for k in range(2):
            for step, way, blocks in ways:
                b = blocks[k]
                send(s.at[h, 2, b], f.at[h, way, k], f_sem.at[h, way, k], {a2: shifted(a2, step)})

    def send_near(h, way):
        a2 = RINGS[h][1]
        step, _, blocks = ways[way]
        g = 1 if way == 0 else 3
        for b in (2, 1, 3, 0):
            if b not in blocks:
                send(s.at[h, g, b], n1.at[h, way, b], n_sem.at[h, way, b], {a2: shifted(a2, step)})

    def pass_on(h, k):
        a2 = RINGS[h][1]
        for step, way, blocks in ways:
            b = blocks[k]
            g = 1 if way == 0 else 3
            landed(f.at[h, way, k], f_sem.at[h, way, k])
            s[h, g, b] = bf16(f32(s[h, g, b]) + f32(f[h, way, k]))
            send(s.at[h, g, b], n1.at[h, way, b], n_sem.at[h, way, b], {a2: shifted(a2, step)})

    def collect(h, b):
        for way in range(2):
            landed(n1.at[h, way, b], n_sem.at[h, way, b])
        t[h, b] = bf16(f32(s[h, 0, b]) + f32(n1[h, 0, b]) + f32(n1[h, 1, b]))

    def send_far2(h):
        a1 = RINGS[h][0]
        for step, way in ((1, 0), (-1, 1)):
            send(t.at[h, 2, pl.ds(way * half, half)], f2.at[h, way], f2_sem.at[h, way], {a1: shifted(a1, step)})

    def pass_on2(h):
        a1 = RINGS[h][0]
        for step, way in ((1, 0), (-1, 1)):
            b = 1 if way == 0 else 3
            piece = pl.ds(way * half, half)
            landed(f2.at[h, way], f2_sem.at[h, way])
            t[h, b, piece] = bf16(f32(t[h, b, piece]) + f32(f2[h, way]))
            send(t.at[h, b], n2.at[h, way], n2_sem.at[h, way], {a1: shifted(a1, step)})

    def finish_plane(h):
        for way in range(2):
            landed(n2.at[h, way], n2_sem.at[h, way])
        for part in range(2):
            piece = pl.ds(part * half, half)
            r[2 * h + part] = bf16(f32(t[h, 0, piece]) + f32(n2[h, 0, piece]) + f32(n2[h, 1, piece]))

    compute(0, 2)
    compute(1, 2)
    chip_sum(0, 2)
    send_far(0)
    compute(0, 1)
    chip_sum(1, 2)
    send_far(1)
    compute(0, 3)
    chip_sum(0, 1)
    send_near(0, 0)
    compute(1, 1)
    chip_sum(0, 3)
    send_near(0, 1)
    compute(1, 3)
    chip_sum(1, 1)
    send_near(1, 0)
    pass_on(0, 0)
    compute(0, 0)
    chip_sum(1, 3)
    send_near(1, 1)
    pass_on(1, 0)
    compute(1, 0)
    chip_sum(0, 0)
    chip_sum(1, 0)
    pass_on(0, 1), pass_on(1, 1)
    for b in (2, 1, 3, 0):
        for h in range(2):
            collect(h, b)
            if b == 2:
                send_far2(h)
    pass_on2(0), pass_on2(1)
    finish_plane(0), finish_plane(1)

    for by in (1, 2, 3):
        send(r.at[lax.rem(xi + by, 4)], xr.at[by - 1], x_sem.at[by - 1], {"x": shifted("x", by)})
    total = f32(r[xi])
    for by in (1, 2, 3):
        landed(xr.at[by - 1], x_sem.at[by - 1])
        total = total + f32(xr[by - 1])
    ob[c, xi] = bf16(total)
    for by in (1, 2, 3):
        send(ob.at[c, xi], ob.at[c, xi], ox_sem.at[by - 1], {"x": shifted("x", by)})
    send(ob.at[c, xi], ob.at[c, xi], od_sem.at[0], other_core())
    for by in (1, 2, 3):
        source = lax.rem(xi + 4 - by, 4)
        landed(ob.at[c, source], ox_sem.at[by - 1])
        send(ob.at[c, source], ob.at[c, source], od_sem.at[by], other_core())
    for by in range(4):
        landed(ob.at[1 - c, lax.rem(xi + 4 - by, 4)], od_sem.at[by])
    store = pltpu.make_async_copy(ob, out, out_sem)
    store.start()
    store.wait()
    send.drain()


def per_device(tokens, expert_ids, gate_weights, live_counts, w_gate, w_up, w_down):
    count, width = tokens.shape
    depth = w_gate.shape[2]
    rows = count // 4
    dma = pltpu.SemaphoreType.DMA
    bf16, f32 = jnp.bfloat16, jnp.float32
    is_live = jnp.arange(count, dtype=jnp.int32)[None, :] < live_counts[0]
    ids, gates = expert_ids.T, gate_weights.T
    named = (ids[:, None, :] == jnp.arange(8, dtype=jnp.int32)[None, :, None]) & is_live[None]
    meta = jnp.sum(jnp.where(named, gates[:, None, :], 0.0), axis=0)

    vmem = pl.BlockSpec(memory_space=pltpu.VMEM)
    hbm = pl.BlockSpec(memory_space=pl.ANY)
    hidden, loads = pl.pallas_call(
        gather_kernel,
        out_shape=(jax.ShapeDtypeStruct((2, 4, 8 * rows, depth), bf16), jax.ShapeDtypeStruct((8, 128), jnp.int32)),
        in_specs=[vmem, vmem, hbm, hbm],
        out_specs=(vmem, vmem),
        scratch_shapes=[
            pltpu.VMEM((2, 4, 2, 4, rows, width), bf16),
            pltpu.VMEM((width, depth), bf16),
            pltpu.VMEM((width, depth), bf16),
            pltpu.VMEM((4, 4, 8, count), f32),
            pltpu.VMEM((4, 4, count, count), f32),
            dma((2,)),
            dma((80,)),
            dma((2, 4, 4)),
            dma((2, 2)),
            dma((2, 4, 4)),
            dma((4, 4)),
        ],
        compiler_params=pltpu.CompilerParams(
            collective_id=0, has_side_effects=True, vmem_limit_bytes=VMEM_LIMIT
        ),
        name="gather",
    )(tokens, meta, w_gate[0], w_up[0])

    mixed = pl.pallas_call(
        scatter_kernel,
        out_shape=jax.ShapeDtypeStruct((2, 4, rows // 2, width), bf16),
        in_specs=[vmem, hbm],
        out_specs=hbm,
        scratch_shapes=[
            pltpu.VMEM((depth, width), bf16),
            pltpu.VMEM((2, 4, 4, rows, width), bf16),
            pltpu.VMEM((2, 4, 4, rows, width), bf16),
            pltpu.VMEM((2, 4, 4, rows, width), bf16),
            pltpu.VMEM((2, 2, 2, rows, width), bf16),
            pltpu.VMEM((2, 2, 4, rows, width), bf16),
            pltpu.VMEM((2, 4, rows, width), bf16),
            pltpu.VMEM((2, 2, rows // 2, width), bf16),
            pltpu.VMEM((2, 2, rows, width), bf16),
            pltpu.VMEM((4, rows // 2, width), bf16),
            pltpu.VMEM((3, rows // 2, width), bf16),
            pltpu.VMEM((2, 4, rows // 2, width), bf16),
            dma(()),
            dma((64,)),
            dma((2, 4)),
            dma((2, 2, 2)),
            dma((2, 2, 4)),
            dma((2, 2)),
            dma((2, 2)),
            dma((3,)),
            dma((3,)),
            dma((4,)),
            dma(()),
        ],
        compiler_params=pltpu.CompilerParams(
            collective_id=1, has_side_effects=True, vmem_limit_bytes=VMEM_LIMIT
        ),
        name="scatter",
    )(hidden, w_down[0])
    return (mixed.reshape(count, width), loads[:, 0])


def solution(mesh):
    torus = Mesh(mesh.devices.reshape(4, 4, 4, 2), DP + EXPERT)
    in_specs = (
        P(DP, None),
        P(DP, None),
        P(DP, None),
        P(DP),
        P(EXPERT, None, DP),
        P(EXPERT, None, DP),
        P(EXPERT, DP, None),
    )
    out_specs = (P(DP, None), P())
    return jax.shard_map(
        per_device, mesh=torus, in_specs=in_specs, out_specs=out_specs, check_vma=False
    )
```

```python
import functools
import jax
import jax.numpy as jnp
from jax import lax
from jax.experimental import pallas as pl
from jax.experimental.pallas import tpu as pltpu
from jax.sharding import Mesh
from jax.sharding import PartitionSpec as P

MESH = pl.DeviceIdType.MESH
DP = ("z", "y")
EXPERT = ("x", "c")
RINGS = (("y", "z"), ("z", "y"))
ORDERS = (("z", "x", "y"), ("y", "z", "x"), ("x", "y", "z"))
LANES = 128
BY_X = 10
PARTS = (12, 12, 8)
VMEM_LIMIT = 67043328


def shifted(axis, by):
    return lax.rem(lax.axis_index(axis) + by % 4, 4)


def other_core():
    return {"c": 1 - lax.axis_index("c")}


class Sender:
    def __init__(self, sems):
        self.sems, self.copies = sems, []

    def __call__(self, src, dst, recv_sem, where):
        copy = pltpu.make_async_remote_copy(
            src_ref=src,
            dst_ref=dst,
            send_sem=self.sems.at[len(self.copies)],
            recv_sem=recv_sem,
            device_id=where,
            device_id_type=MESH,
        )
        copy.start()
        self.copies.append(copy)

    def drain(self):
        for copy in self.copies:
            copy.wait_send()


def landed(ref, sem):
    pltpu.make_async_copy(ref, ref, sem).wait()


def enter(peers):
    barrier = pltpu.get_barrier_semaphore()
    for peer in peers:
        pl.semaphore_signal(barrier, inc=1, device_id=peer, device_id_type=MESH)
    pl.semaphore_wait(barrier, len(peers))


def gather_kernel(
    tok, meta, wg_hbm, wu_hbm, hid, loads, x, wg, wu, m, wcol,
    wsem, send_sem, blk_sem, half_sem, side_sem, swap_sem, meta_sem,
):
    c, xi = lax.axis_index("c"), lax.axis_index("x")
    expert = xi * 2 + c
    parity = lax.rem(xi, 2)
    loads_in = [pltpu.make_async_copy(wg_hbm, wg, wsem.at[0]), pltpu.make_async_copy(wu_hbm, wu, wsem.at[1])]
    for copy in loads_in:
        copy.start()
    rows, width = x.shape[4], x.shape[5]
    half = rows // 2
    by_x = BY_X * LANES
    by_plane = width - by_x
    mine = pl.ds(pl.multiple_of(parity * by_x, LANES), by_plane)
    given = pl.ds(pl.multiple_of(parity * by_plane, LANES), by_x)
    taken = pl.ds(pl.multiple_of((1 - parity) * by_plane, LANES), by_x)
    peers = [(i, j) for i in range(4) for j in range(4) if (i, j) != (0, 0)]
    enter(
        [other_core()]
        + [{"x": shifted("x", 1)}, {"x": shifted("x", -1)}]
        + [{"z": shifted("z", i), "y": shifted("y", j)} for i, j in peers]
    )
    send = Sender(send_sem)

    def own_rows(h, o):
        owner = c if o == 0 else 1 - c
        return pl.ds(pl.multiple_of(owner * (2 * rows) + h * rows, rows), rows)

    for h in range(2):
        own = tok.at[own_rows(h, 0), mine]
        a1, a2 = RINGS[h]
        send(own, x.at[h, 0, 3, 0, :, mine], blk_sem.at[h, 0, 3], {a1: shifted(a1, 1)})
        send(own, x.at[h, 0, 1, 0, :, mine], blk_sem.at[h, 0, 1], {a1: shifted(a1, -1)})
    for h in range(2):
        own = tok.at[own_rows(h, 0), mine]
        a1, a2 = RINGS[h]
        send(own, x.at[h, 3, 0, 0, :, mine], blk_sem.at[h, 3, 0], {a2: shifted(a2, 1)})
        send(own, x.at[h, 1, 0, 0, :, mine], blk_sem.at[h, 1, 0], {a2: shifted(a2, -1)})
    for i, j in peers:
        at = (-i % 4, -j % 4)
        send(meta, m.at[at], meta_sem.at[at], {"z": shifted("z", i), "y": shifted("y", j)})
    m[0, 0] = meta[...]
    for h in range(2):
        for o in range(2):
            x[h, 0, 0, o] = tok[own_rows(h, o), :]

    def aside(h, g, b):
        step = 1 if (b // 2 + g // 2 + h) % 2 == 0 else -1
        part = x.at[h, g, b, 0, :, given]
        send(part, part, side_sem.at[h, g, b], {"x": shifted("x", step)})

    def swap(h, g, b):
        landed(x.at[h, g, b, 0, :, taken], side_sem.at[h, g, b])
        send(x.at[h, g, b, 0], x.at[h, g, b, 1], swap_sem.at[h, g, b], other_core())

    def spread(h, b):
        a2 = RINGS[h][1]
        part = x.at[h, 0, b, 0, :, mine]
        send(part, x.at[h, 3, b, 0, :, mine], blk_sem.at[h, 3, b], {a2: shifted(a2, 1)})
        send(part, x.at[h, 1, b, 0, :, mine], blk_sem.at[h, 1, b], {a2: shifted(a2, -1)})
        aside(h, 0, b)

    def near(h):
        a1 = RINGS[h][0]
        for b, step, part in ((3, 1, 0), (1, -1, 1)):
            landed(x.at[h, 0, b, 0, :, mine], blk_sem.at[h, 0, b])
            piece = pl.ds(part * half, half)
            send(
                x.at[h, 0, b, 0, piece, mine],
                x.at[h, 0, 2, 0, piece, mine],
                half_sem.at[h, part],
                {a1: shifted(a1, step)},
            )
        for b in (3, 1):
            spread(h, b)

    def far(h):
        for part in range(2):
            landed(x.at[h, 0, 2, 0, pl.ds(part * half, half), mine], half_sem.at[h, part])
        spread(h, 2)

    def onward(h, b):
        a2 = RINGS[h][1]
        for g, step, passes in ((3, 1, (0, 2)), (1, -1, (3, 1))):
            part = x.at[h, g, b, 0, :, mine]
            landed(part, blk_sem.at[h, g, b])
            if b in passes:
                send(part, x.at[h, 2, b, 0, :, mine], blk_sem.at[h, 2, b], {a2: shifted(a2, step)})
            aside(h, g, b)

    def last(h, b):
        landed(x.at[h, 2, b, 0, :, mine], blk_sem.at[h, 2, b])
        aside(h, 2, b)

    def weigh():
        for i, j in peers:
            landed(m.at[i, j], meta_sem.at[i, j])
        total = jnp.zeros(m.shape[2:], jnp.float32)
        for i in range(4):
            for j in range(4):
                total = total + jnp.where(m[i, j] > 0.0, 1.0, 0.0)
                row = m[i, j, pl.ds(expert, 1), :]
                wcol[i, j] = jnp.transpose(jnp.broadcast_to(row, (row.shape[1], row.shape[1])))
        loads[...] = jnp.broadcast_to(jnp.sum(total, axis=1, keepdims=True), loads.shape).astype(jnp.int32)

    def compute(blocks):
        places, parts = [], []
        for h, g, b in blocks:
            if (g, b) != (0, 0):
                landed(x.at[h, g, b, 1], swap_sem.at[h, g, b])
            at = (g, b) if h == 0 else (b, g)
            for o in range(2):
                parts.append(wcol[at[0], at[1], own_rows(h, o), :])
                for k in range(2):
                    places.append((*at, lax.rem(2 * h + k + 4 - xi, 4), o))
        weight = jnp.concatenate(parts, axis=0)
        weight = jnp.concatenate([weight, weight], axis=1)

        @pl.loop(0, 2)
        def _(n):
            cols = pl.ds(pl.multiple_of(n * 256, 256), 256)
            lhs = jnp.concatenate([x[block].reshape(2 * rows, width) for block in blocks], axis=0)
            gate = jnp.dot(lhs, wg[:, cols], preferred_element_type=jnp.float32)
            up = jnp.dot(lhs, wu[:, cols], preferred_element_type=jnp.float32)
            act = (gate / (1.0 + jnp.exp(-gate)) * up * weight).astype(jnp.bfloat16)
            for k, place in enumerate(places):
                hid[(*place, slice(None), cols)] = act[k * half : (k + 1) * half]

    both = lambda g, b: [(0, g, b), (1, g, b)]
    near(0), near(1)
    far(0), far(1)
    onward(0, 0), onward(1, 0)
    weigh()
    for copy in loads_in:
        copy.wait()
    swap(0, 0, 3), swap(1, 0, 3), swap(0, 0, 1), swap(1, 0, 1)
    onward(0, 3), onward(1, 3)
    swap(0, 0, 2), swap(1, 0, 2)
    compute(both(0, 3) + both(0, 1))
    for h in range(2):
        swap(h, 3, 0), swap(h, 1, 0)
    onward(0, 1), onward(1, 1)
    compute(both(0, 0) + both(0, 2))
    last(0, 0), last(1, 0)
    for h in range(2):
        swap(h, 3, 3), swap(h, 1, 3)
    compute(both(3, 0) + both(1, 0))
    onward(0, 2), onward(1, 2)
    last(0, 3), last(1, 3)
    for h in range(2):
        swap(h, 3, 1), swap(h, 1, 1)
    compute(both(3, 3) + both(1, 3))
    last(0, 1), last(1, 1)
    swap(0, 2, 0), swap(1, 2, 0)
    for h in range(2):
        swap(h, 3, 2), swap(h, 1, 2)
    compute(both(3, 1) + both(1, 1))
    last(0, 2), last(1, 2)
    swap(0, 2, 3), swap(1, 2, 3)
    swap(0, 2, 1), swap(1, 2, 1)
    compute(both(3, 2) + both(1, 2))
    swap(0, 2, 2), swap(1, 2, 2)
    compute(both(2, 0) + both(2, 3))
    compute(both(2, 1) + both(2, 2))
    send.drain()


WAYS = ((1, 1, (2, 0)), (-1, 3, (1, 3)))


class Level:
    def __init__(self, send, axis, src, far, near, far_sem, near_sem):
        self.send, self.axis, self.src = send, axis, src
        self.far, self.near, self.far_sem, self.near_sem = far, near, far_sem, near_sem

    def send_far(self):
        for k in range(2):
            for way, (step, _, blocks) in enumerate(WAYS):
                self.send(
                    self.src(2, blocks[k]), self.far(way, k), self.far_sem.at[way, k], {self.axis: shifted(self.axis, step)}
                )

    def send_near(self, way, b):
        step, g, _ = WAYS[way]
        self.send(self.src(g, b), self.near(way, b), self.near_sem.at[way, b], {self.axis: shifted(self.axis, step)})

    def send_direct(self, way):
        for b in (2, 1, 3, 0):
            if b not in WAYS[way][2]:
                self.send_near(way, b)

    def pass_on(self, k):
        for way, (_, g, blocks) in enumerate(WAYS):
            landed(self.far(way, k), self.far_sem.at[way, k])
            add_up(self.src(g, blocks[k]), [self.src(g, blocks[k]), self.far(way, k)])
            self.send_near(way, blocks[k])

    def collect(self, b, out):
        for way in range(2):
            landed(self.near(way, b), self.near_sem.at[way, b])
        add_up(out, [self.src(0, b), self.near(0, b), self.near(1, b)])


def add_up(out, terms):
    total = terms[0][...].astype(jnp.float32)
    for term in terms[1:]:
        total = total + term[...].astype(jnp.float32)
    out[...] = total.astype(jnp.bfloat16)


def scatter_kernel(
    hid, wd_hbm, out, wd, s, p, l, f1, n1, t, f2, n2, u, f3, n3, ob,
    wsem, send_sem, l_sem, f1_sem, n1_sem, f2_sem, n2_sem, f3_sem, n3_sem, ox_sem, od_sem, out_sem,
):
    c, xi = lax.axis_index("c"), lax.axis_index("x")
    load = pltpu.make_async_copy(wd_hbm, wd, wsem)
    load.start()
    enter([other_core()] + [{a: shifted(a, by)} for a in ("x", "y", "z") for by in (1, -1)] + [{"x": shifted("x", 2)}])
    send = Sender(send_sem)
    load.wait()
    every = range(3)
    sizes = [n * LANES for n in PARTS]
    starts = [sum(sizes[:q]) for q in every]
    span = [pl.ds(0, n) for n in sizes]
    first = [
        Level(
            send,
            ORDERS[q][0],
            lambda g, b, q=q: s.at[q, g, b, :, :, span[q]],
            lambda way, k, q=q: f1.at[q, way, k, :, :, span[q]],
            lambda way, b, q=q: n1.at[q, way, b, :, :, span[q]],
            f1_sem.at[q],
            n1_sem.at[q],
        )
        for q in every
    ]
    second = [
        Level(
            send,
            ORDERS[q][1],
            lambda g, b, q=q: t.at[q, g, b, :, span[q]],
            lambda way, k, q=q: f2.at[q, way, k, :, span[q]],
            lambda way, b, q=q: n2.at[q, way, b, :, span[q]],
            f2_sem.at[q],
            n2_sem.at[q],
        )
        for q in every
    ]

    def compute(q, i):
        pieces = []
        for o in range(2):
            for j in range(4):
                for k in range(4):
                    at = dict(zip(ORDERS[q], (i, j, k)))
                    pieces.append((at["z"], at["y"], at["x"], o))
        for lo in range(0, sizes[q], 512):
            n = min(512, sizes[q] - lo)
            lhs = jnp.concatenate([hid[piece] for piece in pieces], axis=0)
            y = jnp.dot(lhs, wd[:, starts[q] + lo : starts[q] + lo + n], preferred_element_type=jnp.float32)
            y = y.astype(jnp.bfloat16).reshape(2, 4, 4, lhs.shape[0] // 32, n)
            s[q, i, :, :, :, lo : lo + n] = y[0]
            p[q, i, :, :, :, lo : lo + n] = y[1]
        send(p.at[q, i, :, :, :, span[q]], l.at[q, i, :, :, :, span[q]], l_sem.at[q, i], other_core())

    def chip_sum(q, i):
        landed(l.at[q, i, :, :, :, span[q]], l_sem.at[q, i])

        @pl.loop(0, 4)
        def _(j):
            add_up(s.at[q, i, j, :, :, span[q]], [s.at[q, i, j, :, :, span[q]], l.at[q, i, j, :, :, span[q]]])

    for q in every:
        compute(q, 2)
    for q in every:
        chip_sum(q, 2)
        first[q].send_far()
    for q in every:
        compute(q, 1)
    for q in every:
        chip_sum(q, 1)
        first[q].send_direct(0)
    for q in every:
        compute(q, 3)
    for q in every:
        chip_sum(q, 3)
        first[q].send_direct(1)
    for q in every:
        first[q].pass_on(0)
    for q in every:
        compute(q, 0)
    for q in every:
        first[q].pass_on(1)
    for q in every:
        chip_sum(q, 0)
    down = lambda q, b: first[q].collect(b, t.at[q, b, :, :, span[q]])
    for q in every:
        down(q, 2)
        second[q].send_far()
    for q in every:
        down(q, 1)
        second[q].send_direct(0)
        down(q, 3)
        second[q].send_direct(1)
    for q in every:
        second[q].pass_on(0)
    for q in every:
        down(q, 0)
    for q in every:
        second[q].pass_on(1)
    ends = [u.at[q, :, :, span[q]] for q in every]
    for q in every:
        a = ORDERS[q][2]
        second[q].collect(2, ends[q].at[2])
        send(ends[q].at[2], f3.at[q, :, span[q]], f3_sem.at[q], {a: shifted(a, 1)})
    for q in every:
        a = ORDERS[q][2]
        second[q].collect(3, ends[q].at[3])
        send(ends[q].at[3], n3.at[q, 1, :, span[q]], n3_sem.at[q, 1], {a: shifted(a, -1)})
    for q in every:
        a = ORDERS[q][2]
        second[q].collect(1, ends[q].at[1])
        landed(f3.at[q, :, span[q]], f3_sem.at[q])
        add_up(ends[q].at[1], [ends[q].at[1], f3.at[q, :, span[q]]])
        send(ends[q].at[1], n3.at[q, 0, :, span[q]], n3_sem.at[q, 0], {a: shifted(a, 1)})
    for q in every:
        second[q].collect(0, ends[q].at[0])
    for q in every:
        for way in range(2):
            landed(n3.at[q, way, :, span[q]], n3_sem.at[q, way])
        cols = pl.ds(starts[q], sizes[q])
        done = ob.at[c, xi, :, cols]
        add_up(done, [ends[q].at[0], n3.at[q, 0, :, span[q]], n3.at[q, 1, :, span[q]]])
        for by in (2, 1, 3):
            send(done, done, ox_sem.at[q, by - 1], {"x": shifted("x", by)})
        send(done, done, od_sem.at[q, 0], other_core())
    for q in every:
        cols = pl.ds(starts[q], sizes[q])
        for by in (1, 3, 2):
            part = ob.at[c, lax.rem(xi + 4 - by, 4), :, cols]
            landed(part, ox_sem.at[q, by - 1])
            send(part, part, od_sem.at[q, by], other_core())
    for q in every:
        for by in range(4):
            landed(ob.at[1 - c, lax.rem(xi + 4 - by, 4), :, pl.ds(starts[q], sizes[q])], od_sem.at[q, by])
    store = pltpu.make_async_copy(ob, out, out_sem)
    store.start()
    store.wait()
    send.drain()


def per_device(tokens, expert_ids, gate_weights, live_counts, w_gate, w_up, w_down):
    count, width = tokens.shape
    depth = w_gate.shape[2]
    rows = count // 4
    half = rows // 2
    dma = pltpu.SemaphoreType.DMA
    bf16, f32 = jnp.bfloat16, jnp.float32
    is_live = jnp.arange(count, dtype=jnp.int32)[None, :] < live_counts[0]
    ids, gates = expert_ids.T, gate_weights.T
    named = (ids[:, None, :] == jnp.arange(8, dtype=jnp.int32)[None, :, None]) & is_live[None]
    meta = jnp.sum(jnp.where(named, gates[:, None, :], 0.0), axis=0)

    vmem = pl.BlockSpec(memory_space=pltpu.VMEM)
    hbm = pl.BlockSpec(memory_space=pl.ANY)
    hidden, loads = pl.pallas_call(
        gather_kernel,
        out_shape=(
            jax.ShapeDtypeStruct((4, 4, 4, 2, half, depth), bf16),
            jax.ShapeDtypeStruct((8, 128), jnp.int32),
        ),
        in_specs=[vmem, vmem, hbm, hbm],
        out_specs=(vmem, vmem),
        scratch_shapes=[
            pltpu.VMEM((2, 4, 4, 2, rows, width), bf16),
            pltpu.VMEM((width, depth), bf16),
            pltpu.VMEM((width, depth), bf16),
            pltpu.VMEM((4, 4, 8, count), f32),
            pltpu.VMEM((4, 4, count, count), f32),
            dma((2,)),
            dma((112,)),
            dma((2, 4, 4)),
            dma((2, 2)),
            dma((2, 4, 4)),
            dma((2, 4, 4)),
            dma((4, 4)),
        ],
        compiler_params=pltpu.CompilerParams(
            collective_id=0, has_side_effects=True, vmem_limit_bytes=VMEM_LIMIT
        ),
        name="gather",
    )(tokens, meta, w_gate[0], w_up[0])

    broad = max(PARTS) * LANES
    block = lambda *dims: pltpu.VMEM((3, *dims, half, broad), bf16)
    mixed = pl.pallas_call(
        scatter_kernel,
        out_shape=jax.ShapeDtypeStruct((2, 4, half, width), bf16),
        in_specs=[vmem, hbm],
        out_specs=hbm,
        scratch_shapes=[
            pltpu.VMEM((depth, width), bf16),
            block(4, 4, 4),
            block(4, 4, 4),
            block(4, 4, 4),
            block(2, 2, 4),
            block(2, 4, 4),
            block(4, 4),
            block(2, 2),
            block(2, 4),
            block(4),
            block(),
            block(2),
            pltpu.VMEM((2, 4, half, width), bf16),
            dma(()),
            dma((128,)),
            dma((3, 4)),
            dma((3, 2, 2)),
            dma((3, 2, 4)),
            dma((3, 2, 2)),
            dma((3, 2, 4)),
            dma((3,)),
            dma((3, 2)),
            dma((3, 3)),
            dma((3, 4)),
            dma(()),
        ],
        compiler_params=pltpu.CompilerParams(
            collective_id=1, has_side_effects=True, vmem_limit_bytes=VMEM_LIMIT
        ),
        name="scatter",
    )(hidden, w_down[0])
    return (mixed.reshape(count, width), loads[:, 0])


def solution(mesh):
    torus = Mesh(mesh.devices.reshape(4, 4, 4, 2), DP + EXPERT)
    in_specs = (
        P(DP, None),
        P(DP, None),
        P(DP, None),
        P(DP),
        P(EXPERT, None, DP),
        P(EXPERT, None, DP),
        P(EXPERT, DP, None),
    )
    out_specs = (P(DP, None), P())
    return jax.shard_map(
        per_device, mesh=torus, in_specs=in_specs, out_specs=out_specs, check_vma=False
    )
```

```python
import functools
import math
import jax
import jax.numpy as jnp
from jax import lax
from jax.experimental import pallas as pl
from jax.experimental.pallas import tpu as pltpu
from jax.sharding import Mesh
from jax.sharding import PartitionSpec as P

MESH = pl.DeviceIdType.MESH
DP = ("z", "y")
EXPERT = ("x", "c")
RINGS = (("y", "z"), ("z", "y"))
ORDERS = (("z", "x", "y"), ("y", "z", "x"), ("x", "y", "z"))
LANES = 128
BY_X = 12
PARTS = (12, 12, 8)
STREAMS = 2
VMEM_LIMIT = 67043328


def shifted(axis, by):
    return lax.rem(lax.axis_index(axis) + by % 4, 4)


def other_core():
    return {"c": 1 - lax.axis_index("c")}


class Sender:
    def __init__(self, sem):
        self.sem, self.size = sem, 0

    def __call__(self, src, dst, recv_sem, where):
        self.size += math.prod(src.shape)
        pltpu.make_async_remote_copy(
            src_ref=src, dst_ref=dst, send_sem=self.sem, recv_sem=recv_sem, device_id=where, device_id_type=MESH
        ).start()

    def drain(self, alike):
        assert math.prod(alike.shape) == self.size
        landed(alike, self.sem)


def landed(ref, sem):
    pltpu.make_async_copy(ref, ref, sem).wait()


def enter(peers):
    barrier = pltpu.get_barrier_semaphore()
    for peer in peers:
        pl.semaphore_signal(barrier, inc=1, device_id=peer, device_id_type=MESH)
    pl.semaphore_wait(barrier, len(peers))


class Gather:
    def __init__(self, send, tok, x, base, sems):
        self.send, self.tok, self.x, self.base = send, tok, x, base
        self.near_sem, self.half_sem, self.on_sem, self.side0_sem, self.side_sem, self.last_sem, self.swap_sem = sems
        self.rows, self.width = x.shape[4], x.shape[5]
        parity = lax.rem(lax.axis_index("x"), 2)
        by_x = BY_X * LANES
        by_plane = self.width - by_x
        at = lambda place, size: pl.ds(pl.multiple_of(place, LANES), size)
        self.mine = at(parity * by_x, by_plane)
        self.halves = [at(parity * by_x + n * (by_plane // 2), by_plane // 2) for n in range(2)]
        self.given = at(parity * by_plane, by_x)
        self.taken = at((1 - parity) * by_plane, by_x)

    def own_rows(self, h, o):
        c = lax.axis_index("c")
        owner = c if o == 0 else 1 - c
        start = owner * (self.tok.shape[0] // 2) + self.base + h * self.rows
        return pl.ds(pl.multiple_of(start, self.rows), self.rows)

    def start(self):
        for ring in range(2):
            for h in range(2):
                own = self.tok.at[self.own_rows(h, 0), self.mine]
                a = RINGS[h][ring]
                for step, off in ((1, 3), (-1, 1)):
                    g, b = (0, off) if ring == 0 else (off, 0)
                    to = self.x.at[h, g, b, 0, :, self.mine]
                    sem = self.near_sem.at[h] if ring == 0 else self.on_sem.at[h, 0]
                    self.send(own, to, sem, {a: shifted(a, step)})

    def fill(self):
        for h in range(2):
            for o in range(2):
                self.x[h, 0, 0, o] = self.tok[self.own_rows(h, o), :]

    def aside(self, h, g, b):
        step = 1 if (b // 2 + g // 2 + h) % 2 == 0 else -1
        part = self.x.at[h, g, b, 0, :, self.given]
        sem = self.side0_sem.at[h, int(b == 2)] if g == 0 else self.side_sem.at[h, b]
        self.send(part, part, sem, {"x": shifted("x", step)})

    def swap(self, h, g, b):
        chunk = [(g, b) in pairs for pairs in CHUNKS].index(True)
        self.send(self.x.at[h, g, b, 0], self.x.at[h, g, b, 1], self.swap_sem.at[chunk], other_core())

    passes = {3: (1, (0, 2)), 1: (-1, (3, 1))}

    def forward(self, h, g, b, cols):
        step, blocks = self.passes[g]
        if b in blocks:
            a2 = RINGS[h][1]
            to = self.x.at[h, 2, b, 0, :, cols]
            self.send(self.x.at[h, g, b, 0, :, cols], to, self.last_sem.at[h, b], {a2: shifted(a2, step)})

    def joined_near(self, h):
        landed(self.x.at[h, 0, pl.ds(0, 2), 0, :, self.taken], self.side0_sem.at[h, 0])
        self.swap(h, 0, 3)
        self.swap(h, 0, 1)

    def joined_far(self, h):
        landed(self.x.at[h, 0, 2, 0, :, self.taken], self.side0_sem.at[h, 1])
        self.swap(h, 0, 2)

    def joined(self, h, b):
        landed(self.x.at[h, pl.ds(0, 2), b, 0, :, self.taken], self.side_sem.at[h, b])
        for g in (3, 1):
            self.forward(h, g, b, self.taken)
        for g in (3, 1):
            self.swap(h, g, b)

    def spread(self, h, b):
        a2 = RINGS[h][1]
        for step, g in ((1, 3), (-1, 1)):
            to = self.x.at[h, g, b, 0, :, self.mine]
            self.send(self.x.at[h, 0, b, 0, :, self.mine], to, self.on_sem.at[h, b], {a2: shifted(a2, step)})
        self.aside(h, 0, b)

    def near(self, h):
        a1 = RINGS[h][0]
        landed(self.x.at[h, 0, pl.ds(0, 2), 0, :, self.mine], self.near_sem.at[h])
        for b, step, part in ((3, 1, 0), (1, -1, 1)):
            cols = self.halves[part]
            to = self.x.at[h, 0, 2, 0, :, cols]
            self.send(self.x.at[h, 0, b, 0, :, cols], to, self.half_sem.at[h], {a1: shifted(a1, step)})
        for b in (3, 1):
            self.spread(h, b)

    def far(self, h):
        landed(self.x.at[h, 0, 2, 0, :, self.mine], self.half_sem.at[h])
        self.spread(h, 2)

    def onward(self, h, b):
        landed(self.x.at[h, pl.ds(0, 2), b, 0, :, self.mine], self.on_sem.at[h, b])
        for g in (3, 1):
            self.forward(h, g, b, self.mine)
        for g in (3, 1):
            self.aside(h, g, b)

    def last(self, h, b):
        landed(self.x.at[h, 2, b, 0], self.last_sem.at[h, b])
        self.swap(h, 2, b)

    def compute(self, chunk, wg, wu, wcol, hid):
        pairs = CHUNKS[chunk]
        blocks = [(h, g, b) for g, b in pairs for h in range(2)]
        places, parts = [], []
        count = sum(block[1:] != (0, 0) for block in blocks)
        wide = 4 if count % 4 == 0 else 2
        landed(self.x.at[0, pl.ds(0, count // wide), pl.ds(0, wide), 0], self.swap_sem.at[chunk])
        for h, g, b in blocks:
            at = (g, b) if h == 0 else (b, g)
            for o in range(2):
                parts.append(wcol[at[0], at[1], self.own_rows(h, o), :])
                places.append((*at, o, pl.ds(h * self.rows, self.rows)))
        weight = jnp.concatenate(parts, axis=0)
        weight = jnp.concatenate([weight, weight], axis=1)
        rows = self.rows

        @pl.loop(0, 2)
        def _(n):
            cols = pl.ds(pl.multiple_of(n * 256, 256), 256)
            lhs = jnp.concatenate([self.x[block].reshape(2 * rows, self.width) for block in blocks], axis=0)
            gate = jnp.dot(lhs, wg[:, cols], preferred_element_type=jnp.float32)
            up = jnp.dot(lhs, wu[:, cols], preferred_element_type=jnp.float32)
            act = (gate / (1.0 + jnp.exp(-gate)) * up * weight).astype(jnp.bfloat16)
            for k, place in enumerate(places):
                hid[(*place, cols)] = act[k * rows : (k + 1) * rows]


def pass_meta(m, send, sems, stage):
    if stage == 0:
        send(m.at[0, 0], m.at[0, 3], sems.at[0], {"y": shifted("y", 1)})
        send(m.at[0, 0], m.at[0, 1], sems.at[0], {"y": shifted("y", -1)})
    elif stage == 1:
        landed(m.at[0, pl.ds(0, 2)], sems.at[0])
        send(m.at[0, 3], m.at[0, 2], sems.at[1], {"y": shifted("y", 1)})
    elif stage == 2:
        landed(m.at[0, 2], sems.at[1])
        send(m.at[0], m.at[3], sems.at[2], {"z": shifted("z", 1)})
        send(m.at[0], m.at[1], sems.at[2], {"z": shifted("z", -1)})
    else:
        landed(m.at[pl.ds(0, 2)], sems.at[2])
        send(m.at[3], m.at[2], sems.at[3], {"z": shifted("z", 1)})


def weigh(m, sems, wcol, loads):
    expert = lax.axis_index("x") * 2 + lax.axis_index("c")
    landed(m.at[2], sems.at[3])
    total = jnp.zeros(m.shape[2:], jnp.float32)
    for i in range(4):
        for j in range(4):
            total = total + jnp.where(m[i, j] > 0.0, 1.0, 0.0)
            row = m[i, j, pl.ds(expert, 1), :]
            wcol[i, j] = jnp.transpose(jnp.broadcast_to(row, (row.shape[1], row.shape[1])))
    counts = jnp.broadcast_to(jnp.sum(total, axis=1, keepdims=True), total.shape)
    place = lax.broadcasted_iota(jnp.int32, total.shape, 0) == lax.broadcasted_iota(jnp.int32, total.shape, 1)
    loads[...] = jnp.sum(jnp.where(place, counts, 0.0), axis=0, keepdims=True).astype(jnp.int32)


WAYS = ((1, 1, (2, 0)), (-1, 3, (1, 3)))


class Level:
    def __init__(self, send, axis, src, far, near, far_sem, near_sem):
        self.send, self.axis, self.src = send, axis, src
        self.far, self.near, self.far_sem, self.near_sem = far, near, far_sem, near_sem

    def to(self, step):
        return {self.axis: shifted(self.axis, step)}

    def send_far(self):
        for k in range(2):
            for way, (step, _, blocks) in enumerate(WAYS):
                self.send(self.src(2, blocks[k]), self.far.at[way, k], self.far_sem.at[k], self.to(step))

    def send_near(self, way, b):
        step, g, _ = WAYS[way]
        self.send(self.src(g, b), self.near.at[way, b], self.near_sem.at[b], self.to(step))

    def send_direct(self, way):
        for b in (2, 1, 3, 0):
            if b not in WAYS[way][2]:
                self.send_near(way, b)

    def pass_on(self, k):
        landed(self.far.at[:, k], self.far_sem.at[k])
        for way, (_, g, blocks) in enumerate(WAYS):
            add_up(self.src(g, blocks[k]), [self.src(g, blocks[k]), self.far.at[way, k]])
            self.send_near(way, blocks[k])

    def collect(self, b, out):
        landed(self.near.at[:, b], self.near_sem.at[b])
        add_up(out, [self.src(0, b), self.near.at[0, b], self.near.at[1, b]])


def add_up(out, terms):
    total = terms[0][...].astype(jnp.float32)
    for term in terms[1:]:
        total = total + term[...].astype(jnp.float32)
    out[...] = total.astype(jnp.bfloat16)


SIZES = [n * LANES for n in PARTS]
STARTS = [sum(SIZES[:q]) for q in range(3)]
QUARTERS = [n // 4 for n in SIZES]


class Scatter:
    def __init__(self, sends, hid, wd, x, s, ob, bufs, sems):
        self.sends = [Sender(sends.at[n]) for n in range(3)]
        swap, first, send = self.sends
        self.swap, self.send, self.hid, self.wd, self.x, self.s, self.ob = swap, send, hid, wd, x, s, ob
        self.rows = s.shape[2]
        self.sems = sems
        self.first, self.second, self.bufs = [], [], bufs
        for q in range(3):
            f1, n1, t, f2, n2, u, f3, n3 = bufs[q]
            self.first.append(
                Level(first, ORDERS[q][0], functools.partial(self.block, q), f1, n1, sems["f1"].at[q], sems["n1"].at[q])
            )
            if q == 1:
                src = lambda g, b, t=t: t.at[g, :, pl.ds(b * QUARTERS[1], QUARTERS[1])]
            else:
                src = lambda g, b, t=t: t.at[g, b]
            self.second.append(Level(send, ORDERS[q][1], src, f2, n2, sems["f2"].at[q], sems["n2"].at[q]))

    def cols(self, q, dx):
        return pl.ds(STARTS[q] + dx * QUARTERS[q], QUARTERS[q])

    def block(self, q, g, b):
        if q == 0:
            return self.s.at[g, :, :, self.cols(0, b)]
        if q == 1:
            return self.s.at[b, g, :, pl.ds(STARTS[1], SIZES[1])]
        return self.s.at[:, b, :, self.cols(2, g)]

    def group(self, ref, q, i):
        if q == 0:
            return ref.at[i, :, :, :, pl.ds(STARTS[0], SIZES[0])]
        if q == 1:
            return ref.at[:, i, :, :, pl.ds(STARTS[1], SIZES[1])]
        return ref.at[:, :, :, :, self.cols(2, i)]

    def ranks(self, q, i):
        every = range(4)
        if q == 0:
            return [(i, j) for j in every]
        if q == 1:
            return [(j, i) for j in every]
        return [(j, k) for j in every for k in every]

    def put(self, y, o, at, cols):
        y = y.astype(jnp.bfloat16)
        if o == 0:
            self.s[(*at, slice(None), cols)] = y
        else:
            self.x[(0, *at, slice(None), slice(None), cols)] = y.reshape(2, self.rows // 2, y.shape[1])

    def compute(self, q, i):
        xi = lax.axis_index("x")
        ranks, rows, size = self.ranks(q, i), self.rows, QUARTERS[q]
        if q == 2:
            quarter = lax.rem(xi + i, 4)
            for o in range(2):
                lhs = jnp.concatenate([self.hid[(*at, o)] for at in ranks], axis=0)
                rhs = self.wd[:, pl.ds(pl.multiple_of(STARTS[2] + quarter * size, LANES), size)]
                y = jnp.dot(lhs, rhs, preferred_element_type=jnp.float32)
                for n, at in enumerate(ranks):
                    self.put(y[n * rows : (n + 1) * rows], o, at, self.cols(2, i))
        else:
            for two in range(2):
                lhs = jnp.concatenate([self.hid[(*at, o)] for o in range(2) for at in ranks], axis=0)
                lo = STARTS[q] + two * 2 * size
                y = jnp.dot(lhs, self.wd[:, lo : lo + 2 * size], preferred_element_type=jnp.float32)
                for k in range(2):
                    place = STARTS[q] + lax.rem(2 * two + k + 4 - xi, 4) * size
                    cols = pl.ds(pl.multiple_of(place, LANES), size)
                    for n in range(8):
                        piece = y[n * rows : (n + 1) * rows, k * size : (k + 1) * size]
                        self.put(piece, n // 4, ranks[n % 4], cols)
        self.swap(self.group(self.x.at[0], q, i), self.group(self.x.at[1], q, i), self.sems["l"].at[q, i], other_core())

    def chip_sum(self, q, i):
        landed(self.group(self.x.at[1], q, i), self.sems["l"].at[q, i])
        cols = self.cols(2, i) if q == 2 else pl.ds(STARTS[q], SIZES[q])
        for at in self.ranks(q, i):
            own = self.s.at[(*at, slice(None), cols)]
            other = self.x[(1, *at, slice(None), slice(None), cols)]
            other = other.reshape(self.rows, other.shape[2])
            own[...] = (own[...].astype(jnp.float32) + other.astype(jnp.float32)).astype(jnp.bfloat16)

    def drain(self):
        width = self.s.shape[3]
        for send, part in zip(self.sends, (width, width // 4 * 3, width // 32 * 11)):
            send.drain(self.s.at[:, :, :, pl.ds(0, part)])

    def down(self, q, b):
        t = self.bufs[q][2]
        self.first[q].collect(b, t.at[b])

    def end(self, q, k):
        a, sems = ORDERS[q][2], self.sems
        u, f3, n3 = self.bufs[q][5:]
        self.second[q].collect(k, u.at[k])
        if k == 2:
            self.send(u.at[2], f3, sems["f3"].at[q], {a: shifted(a, 1)})
        elif k == 3:
            self.send(u.at[3], n3.at[1], sems["n3"].at[q], {a: shifted(a, -1)})
        elif k == 1:
            landed(f3, sems["f3"].at[q])
            add_up(u.at[1], [u.at[1], f3])
            self.send(u.at[1], n3.at[0], sems["n3"].at[q], {a: shifted(a, 1)})

    def piece(self, q, core, chip):
        return self.ob.at[core, :, pl.ds(pl.multiple_of(STARTS[q] + chip * QUARTERS[q], LANES), QUARTERS[q])]

    def share(self, q):
        c, xi = lax.axis_index("c"), lax.axis_index("x")
        u, _, n3 = self.bufs[q][5:]
        landed(n3, self.sems["n3"].at[q])
        done = self.piece(q, c, xi)
        add_up(done, [u.at[0], n3.at[0], n3.at[1]])
        for by in (2, 1, 3):
            self.send(done, done, self.sems["ox"].at[q, by - 1], {"x": shifted("x", by)})
        self.send(done, done, self.sems["od"].at[q], other_core())

    def pair(self, q, by):
        part = self.piece(q, lax.axis_index("c"), lax.rem(lax.axis_index("x") + 4 - by, 4))
        landed(part, self.sems["ox"].at[q, by - 1])
        self.send(part, part, self.sems["od"].at[q], other_core())

    def close(self, q):
        landed(self.ob.at[1 - lax.axis_index("c"), :, pl.ds(STARTS[q], SIZES[q])], self.sems["od"].at[q])


RECV = ("l", "f1", "n1", "f2", "n2", "f3", "n3", "ox", "od")


def moe_kernel(
    tok, meta, wg_hbm, wu_hbm, wd_hbm, ob, loads, x, wg, wu, wd, m, wcol, hid, s, bufs,
    wsem, send_sem, meta_sem, free_sem, collect_sems, recv,
):
    weights = [
        pltpu.make_async_copy(src, dst, wsem.at[n])
        for n, (src, dst) in enumerate(((wg_hbm, wg), (wu_hbm, wu), (wd_hbm, wd)))
    ]
    for copy in weights:
        copy.start()
    m[0, 0] = meta[...]
    enter([other_core(), {"x": shifted("x", 2)}] + [{a: shifted(a, by)} for a in ("x", "y", "z") for by in (1, -1)])
    send = Sender(send_sem.at[0, 0])
    gather, scatter = [], []
    per = tok.shape[0] // 2 // STREAMS
    for n in range(STREAMS):
        gather.append(
            Gather(
                Sender(send_sem.at[n, 1]), tok, x.at[n], n * per, [ref.at[n] for ref in collect_sems]
            )
        )
        sems = {name: ref.at[n] for name, ref in zip(RECV, recv)}
        parts = [tuple(buf.at[n] for buf in part) for part in bufs]
        scatter.append(Scatter(send_sem.at[n, pl.ds(2, 3)], hid.at[n], wd, x.at[n], s.at[n], ob.at[:, n], parts, sems))

    pass_meta(m, send, meta_sem, 0)
    for each in gather:
        each.fill()
    relay = functools.partial(pass_meta, m, send, meta_sem)
    plan(gather, scatter, (wg, wu, wcol), hid, free_sem, weights, relay, lambda: weigh(m, meta_sem, wcol, loads))
    send.drain(wcol.at[0, pl.ds(0, 1), pl.ds(0, 120)])
    for each in scatter:
        each.drain()


ORDER = (
    2000, 1100, 3010, 3000, 5010, 1200, 5000, 4010, 6010, 5013, 8010, 5011, 4000, 5001,
    1300, 5003, 8000, 7010, 6000, 8013, 8011, 2100, 5012, 7000, 5002, 0, 8003, 9000,
    8001, 9010, 9013, 8012, 10000, 8002, 9011, 3100, 3110, 10010, 9003, 9001, 9012, 9002,
    4100, 5100, 6100, 5110, 10020, 7100, 5101, 6110, 5103, 10030, 8100, 8101, 4110, 5111,
    5113, 8110, 11000, 8103, 12023, 5102, 12021, 12002, 12012, 12022, 9100, 7110, 13023, 15021,
    9101, 5112, 13021, 15020, 8111, 13002, 14000, 13012, 14010, 9110, 8113, 9103, 13022, 14020,
    12001, 8102, 12011, 12020, 10110, 8112, 13001, 13011, 13020, 15000, 12003, 12013, 16020, 9102,
    10120, 9113, 16021, 9112, 17022, 18020, 17021, 13003, 15001, 16000, 13013, 15011, 16010, 16001,
    16011, 19020, 12010, 15010, 9111, 12000, 10100, 10130, 17023, 19021, 17020, 20020, 20021, 11100,
    12123, 12122, 12121, 13000, 17001, 19000, 17002, 18000, 13010, 17011, 19010, 17010, 17012, 18010,
    12102, 17003, 19001, 13122, 13123, 15121, 12112, 13121, 15120, 17013, 19011, 21022, 13102, 21023,
    14100, 20000, 13112, 14110, 20010, 20001, 12101, 21021, 12111, 12120, 12103, 13101, 15100, 12113,
    13111, 15110, 14120, 17000, 21002, 21003, 21000, 13120, 13103, 15101, 16100, 13113, 16110, 15111,
    16101, 16111, 21020, 22020, 20011, 16120, 12100, 12110, 16121, 23023, 23021, 23022, 13110, 17111,
    19110, 21001, 24020, 13100, 17122, 18120, 17123, 17120, 19121, 17102, 18100, 17101, 17112, 18110,
    19100, 21012, 17121, 19120, 17100, 17103, 19101, 20100, 21013, 22000, 17113, 19111, 20120, 20121,
    20110, 21011, 20111, 17110, 21010, 20101, 21102, 21122, 21123, 21112, 23001, 21120, 23002, 23003,
    21110, 21101, 21103, 21121, 22010, 21111, 21113, 24000, 21100, 22100, 23013, 22120, 22110, 23103,
    23011, 23012, 23102, 24010, 23101, 23121, 23122, 24100, 23123, 23113, 23111, 23112, 24120, 24110,
)
CHUNKS = (((0, 0), (0, 3), (0, 1), (0, 2)), ((3, 0), (1, 0), (3, 3), (1, 3)), ((3, 1), (1, 1), (3, 2), (1, 2)), ((2, 0), (2, 3), (2, 1), (2, 2)))


def plan(gather, scatter, weights_in, hid, free_sem, weights, relay, weigh_all):
    def compute(n, k):
        gather[n].compute(k, *weights_in, hid.at[n])

    def begin():
        weigh_all()
        for copy in weights:
            copy.wait()

    def release(n):
        gather[n].send.drain(gather[n].x.at[:, :, :, :, :, pl.ds(0, gather[n].width // 32 * 30)])
        pl.semaphore_signal(free_sem.at[n], inc=1, device_id=other_core(), device_id_type=MESH)
        pl.semaphore_wait(free_sem.at[n], 1)

    steps = (
        (0, begin),
        (1, relay),
        (1, lambda n: gather[n].start()),
        (2, lambda n, h: gather[n].near(h)),
        (2, lambda n, h: gather[n].far(h)),
        (3, lambda n, h, b: gather[n].onward(h, b)),
        (2, lambda n, h: gather[n].joined_near(h)),
        (2, lambda n, h: gather[n].joined_far(h)),
        (3, lambda n, h, b: gather[n].joined(h, b)),
        (3, lambda n, h, b: gather[n].last(h, b)),
        (2, compute),
        (1, release),
        (3, lambda n, q, i: scatter[n].compute(q, i)),
        (3, lambda n, q, i: scatter[n].chip_sum(q, i)),
        (2, lambda n, q: scatter[n].first[q].send_far()),
        (3, lambda n, q, way: scatter[n].first[q].send_direct(way)),
        (3, lambda n, q, k: scatter[n].first[q].pass_on(k)),
        (3, lambda n, q, b: scatter[n].down(q, b)),
        (2, lambda n, q: scatter[n].second[q].send_far()),
        (3, lambda n, q, way: scatter[n].second[q].send_direct(way)),
        (3, lambda n, q, k: scatter[n].second[q].pass_on(k)),
        (3, lambda n, q, k: scatter[n].end(q, k)),
        (2, lambda n, q: scatter[n].share(q)),
        (3, lambda n, q, by: scatter[n].pair(q, by)),
        (2, lambda n, q: scatter[n].close(q)),
    )
    for code in ORDER:
        count, step = steps[code // 1000]
        step(*(code // place % 10 for place in (100, 10, 1)[:count]))


def per_device(tokens, expert_ids, gate_weights, live_counts, w_gate, w_up, w_down):
    count, width = tokens.shape
    depth = w_gate.shape[2]
    rows = count // 2 // STREAMS
    dma = pltpu.SemaphoreType.DMA
    bf16, f32 = jnp.bfloat16, jnp.float32
    is_live = jnp.arange(count, dtype=jnp.int32)[None, :] < live_counts[0]
    ids, gates = expert_ids.T, gate_weights.T
    named = (ids[:, None, :] == jnp.arange(8, dtype=jnp.int32)[None, :, None]) & is_live[None]
    meta = jnp.sum(jnp.where(named, gates[:, None, :], 0.0), axis=0)

    vmem = pl.BlockSpec(memory_space=pltpu.VMEM)
    hbm = pl.BlockSpec(memory_space=pl.ANY)
    n = STREAMS
    bufs = []
    for q in range(3):
        wide = QUARTERS[q]
        one = (rows, 4 * wide) if q == 1 else (4, rows, wide)
        bufs.append(
            [
                pltpu.VMEM(shape, bf16)
                for shape in (
                    (n, 2, 2, *one), (n, 2, 4, *one), (n, 4, *one), (n, 2, 2, rows, wide), (n, 2, 4, rows, wide),
                    (n, 4, rows, wide), (n, rows, wide), (n, 2, rows, wide),
                )
            ]
        )
    mixed, loads = pl.pallas_call(
        moe_kernel,
        out_shape=(
            jax.ShapeDtypeStruct((2, n, rows, width), bf16),
            jax.ShapeDtypeStruct((1, 128), jnp.int32),
        ),
        in_specs=[vmem, vmem, hbm, hbm, hbm],
        out_specs=(vmem, vmem),
        scratch_shapes=[
            pltpu.VMEM((n, 2, 4, 4, 2, rows // 2, width), bf16),
            pltpu.VMEM((width, depth), bf16),
            pltpu.VMEM((width, depth), bf16),
            pltpu.VMEM((depth, width), bf16),
            pltpu.VMEM((4, 4, 8, count), f32),
            pltpu.VMEM((4, 4, count, count), f32),
            pltpu.VMEM((n, 4, 4, 2, rows, depth), bf16),
            pltpu.VMEM((n, 4, 4, rows, width), bf16),
            bufs,
            dma((3,)),
            dma((n, 5)),
            dma((4,)),
            pltpu.SemaphoreType.REGULAR((n,)),
            [
                dma((n, 2)), dma((n, 2)), dma((n, 2, 4)), dma((n, 2, 2)), dma((n, 2, 4)), dma((n, 2, 4)),
                dma((n, len(CHUNKS))),
            ],
            [
                dma((n, 3, 4)), dma((n, 3, 2)), dma((n, 3, 4)), dma((n, 3, 2)), dma((n, 3, 4)),
                dma((n, 3)), dma((n, 3)), dma((n, 3, 3)), dma((n, 3)),
            ],
        ],
        compiler_params=pltpu.CompilerParams(
            collective_id=0, has_side_effects=True, vmem_limit_bytes=VMEM_LIMIT
        ),
        name="moe",
    )(tokens, meta, w_gate[0], w_up[0], w_down[0])
    return (mixed.reshape(count, width), loads[0, :8])


def solution(mesh):
    torus = Mesh(mesh.devices.reshape(4, 4, 4, 2), DP + EXPERT)
    in_specs = (
        P(DP, None),
        P(DP, None),
        P(DP, None),
        P(DP),
        P(EXPERT, None, DP),
        P(EXPERT, None, DP),
        P(EXPERT, DP, None),
    )
    out_specs = (P(DP, None), P())
    return jax.shard_map(
        per_device, mesh=torus, in_specs=in_specs, out_specs=out_specs, check_vma=False
    )
```

```python
import functools
import math
import jax
import jax.numpy as jnp
from jax import lax
from jax.experimental import pallas as pl
from jax.experimental.pallas import tpu as pltpu
from jax.sharding import Mesh
from jax.sharding import PartitionSpec as P

MESH = pl.DeviceIdType.MESH
DP = ("z", "y")
EXPERT = ("x", "c")
RINGS = (("y", "z"), ("z", "y"))
ORDERS = (("z", "x", "y"), ("y", "z", "x"), ("x", "y", "z"))
LANES = 128
BY_X = 12
PARTS = (12, 12, 8)
STREAMS = 2
VMEM_LIMIT = 67043328


def shifted(axis, by):
    return lax.rem(lax.axis_index(axis) + by % 4, 4)


def other_core():
    return {"c": 1 - lax.axis_index("c")}


class Sender:
    def __init__(self, sem):
        self.sem, self.size = sem, 0

    def __call__(self, src, dst, recv_sem, where):
        self.size += math.prod(src.shape)
        pltpu.make_async_remote_copy(
            src_ref=src, dst_ref=dst, send_sem=self.sem, recv_sem=recv_sem, device_id=where, device_id_type=MESH
        ).start()

    def drain(self, alike):
        assert math.prod(alike.shape) == self.size
        landed(alike, self.sem)


def landed(ref, sem):
    pltpu.make_async_copy(ref, ref, sem).wait()


def enter(peers):
    barrier = pltpu.get_barrier_semaphore()
    for peer in peers:
        pl.semaphore_signal(barrier, inc=1, device_id=peer, device_id_type=MESH)
    pl.semaphore_wait(barrier, len(peers))


class Gather:
    def __init__(self, send, tok, x, base, sems):
        self.send, self.tok, self.x, self.base = send, tok, x, base
        self.near_sem, self.half_sem, self.on_sem, self.side0_sem, self.side_sem, self.last_sem, self.swap_sem = sems
        self.rows, self.width = x.shape[4], x.shape[5]
        parity = lax.rem(lax.axis_index("x"), 2)
        by_x = BY_X * LANES
        by_plane = self.width - by_x
        at = lambda place, size: pl.ds(pl.multiple_of(place, LANES), size)
        self.mine = at(parity * by_x, by_plane)
        self.halves = [at(parity * by_x + n * (by_plane // 2), by_plane // 2) for n in range(2)]
        self.given = at(parity * by_plane, by_x)
        self.taken = at((1 - parity) * by_plane, by_x)

    def own_rows(self, h, o):
        c = lax.axis_index("c")
        owner = c if o == 0 else 1 - c
        start = owner * (self.tok.shape[0] // 2) + self.base + h * self.rows
        return pl.ds(pl.multiple_of(start, self.rows), self.rows)

    def start(self):
        for ring in range(2):
            for h in range(2):
                own = self.tok.at[self.own_rows(h, 0), self.mine]
                a = RINGS[h][ring]
                for step, off in ((1, 3), (-1, 1)):
                    g, b = (0, off) if ring == 0 else (off, 0)
                    to = self.x.at[h, g, b, 0, :, self.mine]
                    sem = self.near_sem.at[h] if ring == 0 else self.on_sem.at[h, 0]
                    self.send(own, to, sem, {a: shifted(a, step)})

    def fill(self):
        for h in range(2):
            for o in range(2):
                self.x[h, 0, 0, o] = self.tok[self.own_rows(h, o), :]

    def aside(self, h, g, b):
        step = 1 if (b // 2 + g // 2 + h) % 2 == 0 else -1
        part = self.x.at[h, g, b, 0, :, self.given]
        sem = self.side0_sem.at[h, int(b == 2)] if g == 0 else self.side_sem.at[h, b]
        self.send(part, part, sem, {"x": shifted("x", step)})

    def swap(self, h, g, b):
        chunk = [(g, b) in pairs for pairs in CHUNKS].index(True)
        self.send(self.x.at[h, g, b, 0], self.x.at[h, g, b, 1], self.swap_sem.at[chunk], other_core())

    passes = {3: (1, (0, 2)), 1: (-1, (3, 1))}

    def forward(self, h, g, b, cols):
        step, blocks = self.passes[g]
        if b in blocks:
            a2 = RINGS[h][1]
            to = self.x.at[h, 2, b, 0, :, cols]
            self.send(self.x.at[h, g, b, 0, :, cols], to, self.last_sem.at[h, b], {a2: shifted(a2, step)})

    def joined_near(self, h):
        landed(self.x.at[h, 0, pl.ds(0, 2), 0, :, self.taken], self.side0_sem.at[h, 0])
        self.swap(h, 0, 3)
        self.swap(h, 0, 1)

    def joined_far(self, h):
        landed(self.x.at[h, 0, 2, 0, :, self.taken], self.side0_sem.at[h, 1])
        self.swap(h, 0, 2)

    def joined(self, h, b):
        landed(self.x.at[h, pl.ds(0, 2), b, 0, :, self.taken], self.side_sem.at[h, b])
        for g in (3, 1):
            self.forward(h, g, b, self.taken)
        for g in (3, 1):
            self.swap(h, g, b)

    def spread(self, h, b):
        a2 = RINGS[h][1]
        for step, g in ((1, 3), (-1, 1)):
            to = self.x.at[h, g, b, 0, :, self.mine]
            self.send(self.x.at[h, 0, b, 0, :, self.mine], to, self.on_sem.at[h, b], {a2: shifted(a2, step)})
        self.aside(h, 0, b)

    def near(self, h):
        a1 = RINGS[h][0]
        landed(self.x.at[h, 0, pl.ds(0, 2), 0, :, self.mine], self.near_sem.at[h])
        for b, step, part in ((3, 1, 0), (1, -1, 1)):
            cols = self.halves[part]
            to = self.x.at[h, 0, 2, 0, :, cols]
            self.send(self.x.at[h, 0, b, 0, :, cols], to, self.half_sem.at[h], {a1: shifted(a1, step)})
        for b in (3, 1):
            self.spread(h, b)

    def far(self, h):
        landed(self.x.at[h, 0, 2, 0, :, self.mine], self.half_sem.at[h])
        self.spread(h, 2)

    def onward(self, h, b):
        landed(self.x.at[h, pl.ds(0, 2), b, 0, :, self.mine], self.on_sem.at[h, b])
        for g in (3, 1):
            self.forward(h, g, b, self.mine)
        for g in (3, 1):
            self.aside(h, g, b)

    def last(self, h, b):
        landed(self.x.at[h, 2, b, 0], self.last_sem.at[h, b])
        self.swap(h, 2, b)

    def compute(self, chunk, wg, wu, wcol, hid):
        pairs = CHUNKS[chunk]
        blocks = [(h, g, b) for g, b in pairs for h in range(2)]
        places, parts = [], []
        count = sum(block[1:] != (0, 0) for block in blocks)
        wide = 4 if count % 4 == 0 else 2
        landed(self.x.at[0, pl.ds(0, count // wide), pl.ds(0, wide), 0], self.swap_sem.at[chunk])
        for h, g, b in blocks:
            at = (g, b) if h == 0 else (b, g)
            for o in range(2):
                parts.append(wcol[at[0], at[1], self.own_rows(h, o), :])
                places.append((*at, o, pl.ds(h * self.rows, self.rows)))
        weight = jnp.concatenate(parts, axis=0)
        weight = jnp.concatenate([weight, weight], axis=1)
        rows = self.rows

        @pl.loop(0, 2)
        def _(n):
            cols = pl.ds(pl.multiple_of(n * 256, 256), 256)
            lhs = jnp.concatenate([self.x[block].reshape(2 * rows, self.width) for block in blocks], axis=0)
            gate = jnp.dot(lhs, wg[:, cols], preferred_element_type=jnp.float32)
            up = jnp.dot(lhs, wu[:, cols], preferred_element_type=jnp.float32)
            act = (gate / (1.0 + jnp.exp(-gate)) * up * weight).astype(jnp.bfloat16)
            for k, place in enumerate(places):
                hid[(*place, cols)] = act[k * rows : (k + 1) * rows]


def pass_meta(m, send, sems, stage):
    if stage == 0:
        send(m.at[0, 0], m.at[0, 3], sems.at[0], {"y": shifted("y", 1)})
        send(m.at[0, 0], m.at[0, 1], sems.at[0], {"y": shifted("y", -1)})
    elif stage == 1:
        landed(m.at[0, pl.ds(0, 2)], sems.at[0])
        send(m.at[0, 3], m.at[0, 2], sems.at[1], {"y": shifted("y", 1)})
    elif stage == 2:
        landed(m.at[0, 2], sems.at[1])
        send(m.at[0], m.at[3], sems.at[2], {"z": shifted("z", 1)})
        send(m.at[0], m.at[1], sems.at[2], {"z": shifted("z", -1)})
    else:
        landed(m.at[pl.ds(0, 2)], sems.at[2])
        send(m.at[3], m.at[2], sems.at[3], {"z": shifted("z", 1)})


def weigh(m, sems, wcol, loads):
    expert = lax.axis_index("x") * 2 + lax.axis_index("c")
    landed(m.at[2], sems.at[3])
    total = jnp.zeros(m.shape[2:], jnp.float32)
    for i in range(4):
        for j in range(4):
            total = total + jnp.where(m[i, j] > 0.0, 1.0, 0.0)
            row = m[i, j, pl.ds(expert, 1), :]
            wcol[i, j] = jnp.transpose(jnp.broadcast_to(row, (row.shape[1], row.shape[1])))
    counts = jnp.broadcast_to(jnp.sum(total, axis=1, keepdims=True), total.shape)
    place = lax.broadcasted_iota(jnp.int32, total.shape, 0) == lax.broadcasted_iota(jnp.int32, total.shape, 1)
    loads[...] = jnp.sum(jnp.where(place, counts, 0.0), axis=0, keepdims=True).astype(jnp.int32)


WAYS = ((1, 1, (2, 0)), (-1, 3, (1, 3)))


class Level:
    def __init__(self, send, axis, src, far, near, far_sem, near_sem):
        self.send, self.axis, self.src = send, axis, src
        self.far, self.near, self.far_sem, self.near_sem = far, near, far_sem, near_sem

    def to(self, step):
        return {self.axis: shifted(self.axis, step)}

    def send_far(self):
        for k in range(2):
            for way, (step, _, blocks) in enumerate(WAYS):
                self.send(self.src(2, blocks[k]), self.far.at[way, k], self.far_sem.at[k], self.to(step))

    def send_near(self, way, b):
        step, g, _ = WAYS[way]
        self.send(self.src(g, b), self.near.at[way, b], self.near_sem.at[b], self.to(step))

    def send_direct(self, way):
        for b in (2, 1, 3, 0):
            if b not in WAYS[way][2]:
                self.send_near(way, b)

    def pass_on(self, k):
        landed(self.far.at[:, k], self.far_sem.at[k])
        for way, (_, g, blocks) in enumerate(WAYS):
            add_up(self.src(g, blocks[k]), [self.src(g, blocks[k]), self.far.at[way, k]])
            self.send_near(way, blocks[k])

    def collect(self, b, out):
        landed(self.near.at[:, b], self.near_sem.at[b])
        add_up(out, [self.src(0, b), self.near.at[0, b], self.near.at[1, b]])


def add_up(out, terms):
    total = terms[0][...].astype(jnp.float32)
    for term in terms[1:]:
        total = total + term[...].astype(jnp.float32)
    out[...] = total.astype(jnp.bfloat16)


SIZES = [n * LANES for n in PARTS]
STARTS = [sum(SIZES[:q]) for q in range(3)]
QUARTERS = [n // 4 for n in SIZES]


class Scatter:
    def __init__(self, sends, hid, wd, x, s, ob, bufs, sems):
        self.sends = [Sender(sends.at[n]) for n in range(3)]
        swap, first, send = self.sends
        self.swap, self.send, self.hid, self.wd, self.x, self.s, self.ob = swap, send, hid, wd, x, s, ob
        self.rows = s.shape[2]
        self.sems = sems
        self.first, self.second, self.bufs = [], [], bufs
        for q in range(3):
            f1, n1, t, f2, n2, u, f3, n3 = bufs[q]
            self.first.append(
                Level(first, ORDERS[q][0], functools.partial(self.block, q), f1, n1, sems["f1"].at[q], sems["n1"].at[q])
            )
            if q == 1:
                src = lambda g, b, t=t: t.at[g, :, pl.ds(b * QUARTERS[1], QUARTERS[1])]
            else:
                src = lambda g, b, t=t: t.at[g, b]
            self.second.append(Level(send, ORDERS[q][1], src, f2, n2, sems["f2"].at[q], sems["n2"].at[q]))

    def cols(self, q, dx):
        return pl.ds(STARTS[q] + dx * QUARTERS[q], QUARTERS[q])

    def block(self, q, g, b):
        if q == 0:
            return self.s.at[g, :, :, self.cols(0, b)]
        if q == 1:
            return self.s.at[b, g, :, pl.ds(STARTS[1], SIZES[1])]
        return self.s.at[:, b, :, self.cols(2, g)]

    def group(self, ref, q, i):
        if q == 0:
            return ref.at[i, :, :, :, pl.ds(STARTS[0], SIZES[0])]
        if q == 1:
            return ref.at[:, i, :, :, pl.ds(STARTS[1], SIZES[1])]
        return ref.at[:, :, :, :, self.cols(2, i)]

    def ranks(self, q, i):
        every = range(4)
        if q == 0:
            return [(i, j) for j in every]
        if q == 1:
            return [(j, i) for j in every]
        return [(j, k) for j in every for k in every]

    def put(self, y, o, at, cols):
        y = y.astype(jnp.bfloat16)
        if o == 0:
            self.s[(*at, slice(None), cols)] = y
        else:
            self.x[(0, *at, slice(None), slice(None), cols)] = y.reshape(2, self.rows // 2, y.shape[1])

    def compute(self, q, i):
        xi = lax.axis_index("x")
        ranks, rows, size = self.ranks(q, i), self.rows, QUARTERS[q]
        if q == 2:
            quarter = lax.rem(xi + i, 4)
            for o in range(2):
                lhs = jnp.concatenate([self.hid[(*at, o)] for at in ranks], axis=0)
                rhs = self.wd[:, pl.ds(pl.multiple_of(STARTS[2] + quarter * size, LANES), size)]
                y = jnp.dot(lhs, rhs, preferred_element_type=jnp.float32)
                for n, at in enumerate(ranks):
                    self.put(y[n * rows : (n + 1) * rows], o, at, self.cols(2, i))
        else:
            for two in range(2):
                lhs = jnp.concatenate([self.hid[(*at, o)] for o in range(2) for at in ranks], axis=0)
                lo = STARTS[q] + two * 2 * size
                y = jnp.dot(lhs, self.wd[:, lo : lo + 2 * size], preferred_element_type=jnp.float32)
                for k in range(2):
                    place = STARTS[q] + lax.rem(2 * two + k + 4 - xi, 4) * size
                    cols = pl.ds(pl.multiple_of(place, LANES), size)
                    for n in range(8):
                        piece = y[n * rows : (n + 1) * rows, k * size : (k + 1) * size]
                        self.put(piece, n // 4, ranks[n % 4], cols)
        self.swap(self.group(self.x.at[0], q, i), self.group(self.x.at[1], q, i), self.sems["l"].at[q, i], other_core())

    def chip_sum(self, q, i):
        landed(self.group(self.x.at[1], q, i), self.sems["l"].at[q, i])
        cols = self.cols(2, i) if q == 2 else pl.ds(STARTS[q], SIZES[q])
        for at in self.ranks(q, i):
            own = self.s.at[(*at, slice(None), cols)]
            other = self.x[(1, *at, slice(None), slice(None), cols)]
            other = other.reshape(self.rows, other.shape[2])
            own[...] = (own[...].astype(jnp.float32) + other.astype(jnp.float32)).astype(jnp.bfloat16)

    def drain(self):
        width = self.s.shape[3]
        for send, part in zip(self.sends, (width, width // 4 * 3, width // 32 * 11)):
            send.drain(self.s.at[:, :, :, pl.ds(0, part)])

    def down(self, q, b):
        t = self.bufs[q][2]
        self.first[q].collect(b, t.at[b])

    def end(self, q, k):
        a, sems = ORDERS[q][2], self.sems
        u, f3, n3 = self.bufs[q][5:]
        self.second[q].collect(k, u.at[k])
        if k == 2:
            self.send(u.at[2], f3, sems["f3"].at[q], {a: shifted(a, 1)})
        elif k == 3:
            self.send(u.at[3], n3.at[1], sems["n3"].at[q], {a: shifted(a, -1)})
        elif k == 1:
            landed(f3, sems["f3"].at[q])
            add_up(u.at[1], [u.at[1], f3])
            self.send(u.at[1], n3.at[0], sems["n3"].at[q], {a: shifted(a, 1)})

    def piece(self, q, core, chip):
        return self.ob.at[core, :, pl.ds(pl.multiple_of(STARTS[q] + chip * QUARTERS[q], LANES), QUARTERS[q])]

    def share(self, q):
        c, xi = lax.axis_index("c"), lax.axis_index("x")
        u, _, n3 = self.bufs[q][5:]
        landed(n3, self.sems["n3"].at[q])
        done = self.piece(q, c, xi)
        add_up(done, [u.at[0], n3.at[0], n3.at[1]])
        for by in (2, 1, 3):
            self.send(done, done, self.sems["ox"].at[q, by - 1], {"x": shifted("x", by)})
        self.send(done, done, self.sems["od"].at[q], other_core())

    def pair(self, q, by):
        part = self.piece(q, lax.axis_index("c"), lax.rem(lax.axis_index("x") + 4 - by, 4))
        landed(part, self.sems["ox"].at[q, by - 1])
        self.send(part, part, self.sems["od"].at[q], other_core())

    def close(self, q):
        landed(self.ob.at[1 - lax.axis_index("c"), :, pl.ds(STARTS[q], SIZES[q])], self.sems["od"].at[q])


RECV = ("l", "f1", "n1", "f2", "n2", "f3", "n3", "ox", "od")


def moe_kernel(
    tok, ids, gates, live, wg_hbm, wu_hbm, wd_hbm, ob, loads, x, wg, wu, wd, m, wcol, hid, s, bufs,
    wsem, send_sem, meta_sem, free_sem, collect_sems, recv,
):
    weights = [
        pltpu.make_async_copy(src, dst, wsem.at[n])
        for n, (src, dst) in enumerate(((wg_hbm, wg), (wu_hbm, wu), (wd_hbm, wd)))
    ]
    for copy in weights:
        copy.start()
    count = tok.shape[0]
    token = lax.broadcasted_iota(jnp.int32, (8, count), 1)
    expert = lax.broadcasted_iota(jnp.int32, (8, count), 0)
    meta = jnp.zeros((8, count), jnp.float32)
    for k in range(2):
        named = (jnp.broadcast_to(ids[k : k + 1, :], (8, count)) == expert) & (token < live[0])
        meta = meta + jnp.where(named, jnp.broadcast_to(gates[k : k + 1, :], (8, count)), 0.0)
    m[0, 0] = meta
    enter([other_core(), {"x": shifted("x", 2)}] + [{a: shifted(a, by)} for a in ("x", "y", "z") for by in (1, -1)])
    send = Sender(send_sem.at[0, 0])
    gather, scatter = [], []
    per = tok.shape[0] // 2 // STREAMS
    for n in range(STREAMS):
        gather.append(
            Gather(
                Sender(send_sem.at[n, 1]), tok, x.at[n], n * per, [ref.at[n] for ref in collect_sems]
            )
        )
        sems = {name: ref.at[n] for name, ref in zip(RECV, recv)}
        parts = [tuple(buf.at[n] for buf in part) for part in bufs]
        scatter.append(Scatter(send_sem.at[n, pl.ds(2, 3)], hid.at[n], wd, x.at[n], s.at[n], ob.at[:, n], parts, sems))

    pass_meta(m, send, meta_sem, 0)
    for each in gather:
        each.fill()
    relay = functools.partial(pass_meta, m, send, meta_sem)
    plan(gather, scatter, (wg, wu, wcol), hid, free_sem, weights, relay, lambda: weigh(m, meta_sem, wcol, loads))
    send.drain(wcol.at[0, pl.ds(0, 1), pl.ds(0, 120)])
    for each in scatter:
        each.drain()


ORDER = (
    2000, 1100, 3000, 3010, 1200, 5000, 5010, 4000, 5003, 6010, 6000, 8000, 5001, 4010,
    5011, 1300, 5013, 8010, 7000, 8003, 8001, 2100, 7010, 5002, 5012, 9000, 9010, 8011,
    0, 10000, 8012, 8013, 9003, 9001, 8002, 3110, 5110, 3100, 5100, 10010, 6110, 9002,
    9011, 9012, 9013, 10020, 10030, 6100, 4100, 5103, 5101, 8100, 8110, 4110, 5111, 5113,
    11000, 12022, 12012, 12021, 7100, 12002, 9110, 13022, 14020, 5102, 13012, 14010, 8103, 9100,
    13021, 15020, 12023, 7110, 8101, 13002, 14000, 5112, 12001, 8111, 12011, 10100, 9101, 8113,
    9103, 13001, 15000, 13023, 15021, 16020, 13011, 8102, 15010, 12020, 10110, 13020, 8112, 9113,
    12013, 9111, 16021, 12003, 17022, 18020, 10120, 17023, 17021, 19020, 17020, 9102, 9112, 20020,
    20021, 13003, 15001, 16000, 16001, 19021, 13013, 15011, 16010, 10130, 21022, 21023, 21020, 16011,
    11100, 12122, 12121, 12102, 12112, 12123, 21021, 13122, 14120, 13121, 15120, 12101, 13102, 14100,
    12111, 13112, 14110, 13123, 15121, 12120, 12113, 13101, 15100, 12103, 16120, 13120, 22020, 13111,
    15110, 13113, 15111, 16121, 12000, 13103, 15101, 16100, 12010, 12110, 16110, 13000, 17001, 19000,
    17002, 17003, 19001, 17000, 16101, 18000, 17121, 23023, 13110, 17122, 18120, 23021, 13010, 17012,
    17011, 17013, 19011, 19010, 17123, 18010, 23022, 17120, 19120, 12100, 24020, 19121, 17010, 16111,
    20000, 20001, 13100, 17102, 18100, 17101, 19100, 17112, 18110, 20120, 17100, 21002, 17111, 19110,
    21003, 21000, 20121, 17103, 19101, 20100, 20101, 17110, 20010, 21122, 20011, 21001, 17113, 19111,
    20110, 21120, 21102, 21123, 21012, 21121, 21103, 21010, 20111, 21112, 21101, 22000, 21013, 21100,
    21011, 22120, 21110, 21113, 21111, 22100, 23123, 23001, 23002, 23003, 22010, 23122, 24000, 23121,
    23103, 22110, 24120, 23102, 23101, 23013, 23012, 23011, 24100, 23113, 24010, 23111, 23112, 24110,
)
CHUNKS = (((0, 0), (0, 3), (0, 1), (0, 2)), ((3, 0), (1, 0), (3, 3), (1, 3)), ((3, 1), (1, 1), (3, 2), (1, 2)), ((2, 0), (2, 3), (2, 1), (2, 2)))


def plan(gather, scatter, weights_in, hid, free_sem, weights, relay, weigh_all):
    def compute(n, k):
        gather[n].compute(k, *weights_in, hid.at[n])

    def begin():
        weigh_all()
        for copy in weights:
            copy.wait()

    def release(n):
        gather[n].send.drain(gather[n].x.at[:, :, :, :, :, pl.ds(0, gather[n].width // 32 * 30)])
        pl.semaphore_signal(free_sem.at[n], inc=1, device_id=other_core(), device_id_type=MESH)
        pl.semaphore_wait(free_sem.at[n], 1)

    steps = (
        (0, begin),
        (1, relay),
        (1, lambda n: gather[n].start()),
        (2, lambda n, h: gather[n].near(h)),
        (2, lambda n, h: gather[n].far(h)),
        (3, lambda n, h, b: gather[n].onward(h, b)),
        (2, lambda n, h: gather[n].joined_near(h)),
        (2, lambda n, h: gather[n].joined_far(h)),
        (3, lambda n, h, b: gather[n].joined(h, b)),
        (3, lambda n, h, b: gather[n].last(h, b)),
        (2, compute),
        (1, release),
        (3, lambda n, q, i: scatter[n].compute(q, i)),
        (3, lambda n, q, i: scatter[n].chip_sum(q, i)),
        (2, lambda n, q: scatter[n].first[q].send_far()),
        (3, lambda n, q, way: scatter[n].first[q].send_direct(way)),
        (3, lambda n, q, k: scatter[n].first[q].pass_on(k)),
        (3, lambda n, q, b: scatter[n].down(q, b)),
        (2, lambda n, q: scatter[n].second[q].send_far()),
        (3, lambda n, q, way: scatter[n].second[q].send_direct(way)),
        (3, lambda n, q, k: scatter[n].second[q].pass_on(k)),
        (3, lambda n, q, k: scatter[n].end(q, k)),
        (2, lambda n, q: scatter[n].share(q)),
        (3, lambda n, q, by: scatter[n].pair(q, by)),
        (2, lambda n, q: scatter[n].close(q)),
    )
    for code in ORDER:
        count, step = steps[code // 1000]
        step(*(code // place % 10 for place in (100, 10, 1)[:count]))


def per_device(tokens, expert_ids, gate_weights, live_counts, w_gate, w_up, w_down):
    count, width = tokens.shape
    depth = w_gate.shape[2]
    rows = count // 2 // STREAMS
    dma = pltpu.SemaphoreType.DMA
    bf16, f32 = jnp.bfloat16, jnp.float32
    vmem = pl.BlockSpec(memory_space=pltpu.VMEM)
    hbm = pl.BlockSpec(memory_space=pl.ANY)
    n = STREAMS
    bufs = []
    for q in range(3):
        wide = QUARTERS[q]
        one = (rows, 4 * wide) if q == 1 else (4, rows, wide)
        bufs.append(
            [
                pltpu.VMEM(shape, bf16)
                for shape in (
                    (n, 2, 2, *one), (n, 2, 4, *one), (n, 4, *one), (n, 2, 2, rows, wide), (n, 2, 4, rows, wide),
                    (n, 4, rows, wide), (n, rows, wide), (n, 2, rows, wide),
                )
            ]
        )
    mixed, loads = pl.pallas_call(
        moe_kernel,
        out_shape=(
            jax.ShapeDtypeStruct((2, n, rows, width), bf16),
            jax.ShapeDtypeStruct((1, 128), jnp.int32),
        ),
        in_specs=[vmem, vmem, vmem, pl.BlockSpec(memory_space=pltpu.SMEM), hbm, hbm, hbm],
        out_specs=(vmem, vmem),
        scratch_shapes=[
            pltpu.VMEM((n, 2, 4, 4, 2, rows // 2, width), bf16),
            pltpu.VMEM((width, depth), bf16),
            pltpu.VMEM((width, depth), bf16),
            pltpu.VMEM((depth, width), bf16),
            pltpu.VMEM((4, 4, 8, count), f32),
            pltpu.VMEM((4, 4, count, count), f32),
            pltpu.VMEM((n, 4, 4, 2, rows, depth), bf16),
            pltpu.VMEM((n, 4, 4, rows, width), bf16),
            bufs,
            dma((3,)),
            dma((n, 5)),
            dma((4,)),
            pltpu.SemaphoreType.REGULAR((n,)),
            [
                dma((n, 2)), dma((n, 2)), dma((n, 2, 4)), dma((n, 2, 2)), dma((n, 2, 4)), dma((n, 2, 4)),
                dma((n, len(CHUNKS))),
            ],
            [
                dma((n, 3, 4)), dma((n, 3, 2)), dma((n, 3, 4)), dma((n, 3, 2)), dma((n, 3, 4)),
                dma((n, 3)), dma((n, 3)), dma((n, 3, 3)), dma((n, 3)),
            ],
        ],
        compiler_params=pltpu.CompilerParams(
            collective_id=0, has_side_effects=True, vmem_limit_bytes=VMEM_LIMIT
        ),
        name="moe",
    )(tokens, expert_ids.T, gate_weights.T, live_counts, w_gate[0], w_up[0], w_down[0])
    return (mixed.reshape(count, width), loads[0, :8])


def solution(mesh):
    torus = Mesh(mesh.devices.reshape(4, 4, 4, 2), DP + EXPERT)
    in_specs = (
        P(DP, None),
        P(DP, None),
        P(DP, None),
        P(DP),
        P(EXPERT, None, DP),
        P(EXPERT, None, DP),
        P(EXPERT, DP, None),
    )
    out_specs = (P(DP, None), P())
    return jax.shard_map(
        per_device, mesh=torus, in_specs=in_specs, out_specs=out_specs, check_vma=False
    )
```

```python
import functools
import math
import jax
import jax.numpy as jnp
from jax import lax
from jax.experimental import pallas as pl
from jax.experimental.pallas import tpu as pltpu
from jax.sharding import Mesh
from jax.sharding import PartitionSpec as P

MESH = pl.DeviceIdType.MESH
DP = ("z", "y")
EXPERT = ("x", "c")
RINGS = (("y", "z"), ("z", "y"))
ORDERS = (("z", "x", "y"), ("y", "z", "x"), ("x", "y", "z"))
LANES = 128
BY_X = 12
PARTS = (12, 12, 8)
STREAMS = 2
VMEM_LIMIT = 67043328


def shifted(axis, by):
    return lax.rem(lax.axis_index(axis) + by % 4, 4)


def other_core():
    return {"c": 1 - lax.axis_index("c")}


class Sender:
    def __init__(self, sem):
        self.sem, self.size = sem, 0

    def __call__(self, src, dst, recv_sem, where):
        self.size += math.prod(src.shape)
        pltpu.make_async_remote_copy(
            src_ref=src, dst_ref=dst, send_sem=self.sem, recv_sem=recv_sem, device_id=where, device_id_type=MESH
        ).start()

    def drain(self, alike):
        assert math.prod(alike.shape) == self.size
        landed(alike, self.sem)


def landed(ref, sem):
    pltpu.make_async_copy(ref, ref, sem).wait()


def enter(peers):
    barrier = pltpu.get_barrier_semaphore()
    for peer in peers:
        pl.semaphore_signal(barrier, inc=1, device_id=peer, device_id_type=MESH)
    pl.semaphore_wait(barrier, len(peers))


class Gather:
    def __init__(self, send, tok, x, base, sems):
        self.send, self.tok, self.x, self.base = send, tok, x, base
        self.near_sem, self.half_sem, self.on_sem, self.side0_sem, self.side_sem, self.last_sem, self.swap_sem = sems
        self.rows, self.width = x.shape[4], x.shape[5]
        parity = lax.rem(lax.axis_index("x"), 2)
        by_x = BY_X * LANES
        by_plane = self.width - by_x
        at = lambda place, size: pl.ds(pl.multiple_of(place, LANES), size)
        self.mine = at(parity * by_x, by_plane)
        self.halves = [at(parity * by_x + n * (by_plane // 2), by_plane // 2) for n in range(2)]
        self.given = at(parity * by_plane, by_x)
        self.taken = at((1 - parity) * by_plane, by_x)

    def own_rows(self, h, o):
        c = lax.axis_index("c")
        owner = c if o == 0 else 1 - c
        start = owner * (self.tok.shape[0] // 2) + self.base + h * self.rows
        return pl.ds(pl.multiple_of(start, self.rows), self.rows)

    def start(self):
        for ring in range(2):
            for h in range(2):
                own = self.tok.at[self.own_rows(h, 0), self.mine]
                a = RINGS[h][ring]
                for step, off in ((1, 3), (-1, 1)):
                    g, b = (0, off) if ring == 0 else (off, 0)
                    to = self.x.at[h, g, b, 0, :, self.mine]
                    sem = self.near_sem.at[h] if ring == 0 else self.on_sem.at[h, 0]
                    self.send(own, to, sem, {a: shifted(a, step)})

    def fill(self):
        for h in range(2):
            for o in range(2):
                self.x[h, 0, 0, o] = self.tok[self.own_rows(h, o), :]

    def aside(self, h, g, b):
        step = 1 if (b // 2 + g // 2 + h) % 2 == 0 else -1
        part = self.x.at[h, g, b, 0, :, self.given]
        sem = self.side0_sem.at[h, int(b == 2)] if g == 0 else self.side_sem.at[h, b]
        self.send(part, part, sem, {"x": shifted("x", step)})

    def swap(self, h, g, b):
        chunk = [(g, b) in pairs for pairs in CHUNKS].index(True)
        self.send(self.x.at[h, g, b, 0], self.x.at[h, g, b, 1], self.swap_sem.at[chunk], other_core())

    passes = {3: (1, (0, 2)), 1: (-1, (3, 1))}

    def forward(self, h, g, b, cols):
        step, blocks = self.passes[g]
        if b in blocks:
            a2 = RINGS[h][1]
            to = self.x.at[h, 2, b, 0, :, cols]
            self.send(self.x.at[h, g, b, 0, :, cols], to, self.last_sem.at[h, b], {a2: shifted(a2, step)})

    def joined_near(self, h):
        landed(self.x.at[h, 0, pl.ds(0, 2), 0, :, self.taken], self.side0_sem.at[h, 0])
        self.swap(h, 0, 3)
        self.swap(h, 0, 1)

    def joined_far(self, h):
        landed(self.x.at[h, 0, 2, 0, :, self.taken], self.side0_sem.at[h, 1])
        self.swap(h, 0, 2)

    def joined(self, h, b):
        landed(self.x.at[h, pl.ds(0, 2), b, 0, :, self.taken], self.side_sem.at[h, b])
        for g in (3, 1):
            self.forward(h, g, b, self.taken)
        for g in (3, 1):
            self.swap(h, g, b)

    def spread(self, h, b):
        a2 = RINGS[h][1]
        for step, g in ((1, 3), (-1, 1)):
            to = self.x.at[h, g, b, 0, :, self.mine]
            self.send(self.x.at[h, 0, b, 0, :, self.mine], to, self.on_sem.at[h, b], {a2: shifted(a2, step)})
        self.aside(h, 0, b)

    def near(self, h):
        a1 = RINGS[h][0]
        landed(self.x.at[h, 0, pl.ds(0, 2), 0, :, self.mine], self.near_sem.at[h])
        for b, step, part in ((3, 1, 0), (1, -1, 1)):
            cols = self.halves[part]
            to = self.x.at[h, 0, 2, 0, :, cols]
            self.send(self.x.at[h, 0, b, 0, :, cols], to, self.half_sem.at[h], {a1: shifted(a1, step)})
        for b in (3, 1):
            self.spread(h, b)

    def far(self, h):
        landed(self.x.at[h, 0, 2, 0, :, self.mine], self.half_sem.at[h])
        self.spread(h, 2)

    def onward(self, h, b):
        landed(self.x.at[h, pl.ds(0, 2), b, 0, :, self.mine], self.on_sem.at[h, b])
        for g in (3, 1):
            self.forward(h, g, b, self.mine)
        for g in (3, 1):
            self.aside(h, g, b)

    def last(self, h, b):
        landed(self.x.at[h, 2, b, 0], self.last_sem.at[h, b])
        self.swap(h, 2, b)

    def compute(self, chunk, wg, wu, wcol, hid):
        pairs = CHUNKS[chunk]
        blocks = [(h, g, b) for g, b in pairs for h in range(2)]
        places, parts = [], []
        count = sum(block[1:] != (0, 0) for block in blocks)
        wide = 4 if count % 4 == 0 else 2
        landed(self.x.at[0, pl.ds(0, count // wide), pl.ds(0, wide), 0], self.swap_sem.at[chunk])
        for h, g, b in blocks:
            at = (g, b) if h == 0 else (b, g)
            for o in range(2):
                parts.append(wcol[at[0], at[1], self.own_rows(h, o), :])
                places.append((*at, o, pl.ds(h * self.rows, self.rows)))
        weight = jnp.concatenate(parts, axis=0)
        weight = jnp.concatenate([weight, weight], axis=1)
        rows = self.rows

        @pl.loop(0, 2)
        def _(n):
            cols = pl.ds(pl.multiple_of(n * 256, 256), 256)
            lhs = jnp.concatenate([self.x[block].reshape(2 * rows, self.width) for block in blocks], axis=0)
            gate = jnp.dot(lhs, wg[:, cols], preferred_element_type=jnp.float32)
            up = jnp.dot(lhs, wu[:, cols], preferred_element_type=jnp.float32)
            act = (gate / (1.0 + jnp.exp(-gate)) * up * weight).astype(jnp.bfloat16)
            for k, place in enumerate(places):
                hid[(*place, cols)] = act[k * rows : (k + 1) * rows]


def pass_meta(m, send, sems, stage):
    if stage == 0:
        send(m.at[0, 0], m.at[0, 3], sems.at[0], {"y": shifted("y", 1)})
        send(m.at[0, 0], m.at[0, 1], sems.at[0], {"y": shifted("y", -1)})
    elif stage == 1:
        landed(m.at[0, pl.ds(0, 2)], sems.at[0])
        send(m.at[0, 3], m.at[0, 2], sems.at[1], {"y": shifted("y", 1)})
    elif stage == 2:
        landed(m.at[0, 2], sems.at[1])
        send(m.at[0], m.at[3], sems.at[2], {"z": shifted("z", 1)})
        send(m.at[0], m.at[1], sems.at[2], {"z": shifted("z", -1)})
    else:
        landed(m.at[pl.ds(0, 2)], sems.at[2])
        send(m.at[3], m.at[2], sems.at[3], {"z": shifted("z", 1)})


def weigh(m, sems, wcol, loads):
    expert = lax.axis_index("x") * 2 + lax.axis_index("c")
    landed(m.at[2], sems.at[3])
    total = jnp.zeros(m.shape[2:], jnp.float32)
    for i in range(4):
        for j in range(4):
            total = total + jnp.where(m[i, j] > 0.0, 1.0, 0.0)
            row = m[i, j, pl.ds(expert, 1), :]
            wcol[i, j] = jnp.transpose(jnp.broadcast_to(row, (row.shape[1], row.shape[1])))
    counts = jnp.broadcast_to(jnp.sum(total, axis=1, keepdims=True), total.shape)
    place = lax.broadcasted_iota(jnp.int32, total.shape, 0) == lax.broadcasted_iota(jnp.int32, total.shape, 1)
    loads[...] = jnp.sum(jnp.where(place, counts, 0.0), axis=0, keepdims=True).astype(jnp.int32)


WAYS = ((1, 1, (2, 0)), (-1, 3, (1, 3)))


class Level:
    def __init__(self, send, axis, src, far, near, far_sem, near_sem):
        self.send, self.axis, self.src = send, axis, src
        self.far, self.near, self.far_sem, self.near_sem = far, near, far_sem, near_sem

    def to(self, step):
        return {self.axis: shifted(self.axis, step)}

    def send_far(self):
        for k in range(2):
            for way, (step, _, blocks) in enumerate(WAYS):
                self.send(self.src(2, blocks[k]), self.far.at[way, k], self.far_sem.at[k], self.to(step))

    def send_near(self, way, b):
        step, g, _ = WAYS[way]
        self.send(self.src(g, b), self.near.at[way, b], self.near_sem.at[b], self.to(step))

    def send_direct(self, way):
        for b in (2, 1, 3, 0):
            if b not in WAYS[way][2]:
                self.send_near(way, b)

    def pass_on(self, k):
        landed(self.far.at[:, k], self.far_sem.at[k])
        for way, (_, g, blocks) in enumerate(WAYS):
            add_up(self.src(g, blocks[k]), [self.src(g, blocks[k]), self.far.at[way, k]])
            self.send_near(way, blocks[k])

    def collect(self, b, out):
        landed(self.near.at[:, b], self.near_sem.at[b])
        add_up(out, [self.src(0, b), self.near.at[0, b], self.near.at[1, b]])


def add_up(out, terms):
    total = terms[0][...].astype(jnp.float32)
    for term in terms[1:]:
        total = total + term[...].astype(jnp.float32)
    out[...] = total.astype(jnp.bfloat16)


SIZES = [n * LANES for n in PARTS]
STARTS = [sum(SIZES[:q]) for q in range(3)]
QUARTERS = [n // 4 for n in SIZES]


class Scatter:
    def __init__(self, sends, hid, wd, x, s, ob, bufs, sems):
        self.sends = [Sender(sends.at[n]) for n in range(3)]
        swap, first, send = self.sends
        self.swap, self.send, self.hid, self.wd, self.x, self.s, self.ob = swap, send, hid, wd, x, s, ob
        self.rows = s.shape[2]
        self.sems = sems
        self.first, self.second, self.bufs = [], [], bufs
        for q in range(3):
            f1, n1, t, f2, n2, u, f3, n3 = bufs[q]
            self.first.append(
                Level(first, ORDERS[q][0], functools.partial(self.block, q), f1, n1, sems["f1"].at[q], sems["n1"].at[q])
            )
            if q == 1:
                src = lambda g, b, t=t: t.at[g, :, pl.ds(b * QUARTERS[1], QUARTERS[1])]
            else:
                src = lambda g, b, t=t: t.at[g, b]
            self.second.append(Level(send, ORDERS[q][1], src, f2, n2, sems["f2"].at[q], sems["n2"].at[q]))

    def cols(self, q, dx):
        return pl.ds(STARTS[q] + dx * QUARTERS[q], QUARTERS[q])

    def block(self, q, g, b):
        if q == 0:
            return self.s.at[g, :, :, self.cols(0, b)]
        if q == 1:
            return self.s.at[b, g, :, pl.ds(STARTS[1], SIZES[1])]
        return self.s.at[:, b, :, self.cols(2, g)]

    def group(self, ref, q, i):
        if q == 0:
            return ref.at[i, :, :, :, pl.ds(STARTS[0], SIZES[0])]
        if q == 1:
            return ref.at[:, i, :, :, pl.ds(STARTS[1], SIZES[1])]
        return ref.at[:, :, :, :, self.cols(2, i)]

    def ranks(self, q, i):
        every = range(4)
        if q == 0:
            return [(i, j) for j in every]
        if q == 1:
            return [(j, i) for j in every]
        return [(j, k) for j in every for k in every]

    def put(self, y, o, at, cols):
        y = y.astype(jnp.bfloat16)
        if o == 0:
            self.s[(*at, slice(None), cols)] = y
        else:
            self.x[(0, *at, slice(None), slice(None), cols)] = y.reshape(2, self.rows // 2, y.shape[1])

    def compute(self, q, i):
        xi = lax.axis_index("x")
        ranks, rows, size = self.ranks(q, i), self.rows, QUARTERS[q]
        if q == 2:
            quarter = lax.rem(xi + i, 4)
            for o in range(2):
                lhs = jnp.concatenate([self.hid[(*at, o)] for at in ranks], axis=0)
                rhs = self.wd[:, pl.ds(pl.multiple_of(STARTS[2] + quarter * size, LANES), size)]
                y = jnp.dot(lhs, rhs, preferred_element_type=jnp.float32)
                for n, at in enumerate(ranks):
                    self.put(y[n * rows : (n + 1) * rows], o, at, self.cols(2, i))
        else:
            for two in range(2):
                lhs = jnp.concatenate([self.hid[(*at, o)] for o in range(2) for at in ranks], axis=0)
                lo = STARTS[q] + two * 2 * size
                y = jnp.dot(lhs, self.wd[:, lo : lo + 2 * size], preferred_element_type=jnp.float32)
                for k in range(2):
                    place = STARTS[q] + lax.rem(2 * two + k + 4 - xi, 4) * size
                    cols = pl.ds(pl.multiple_of(place, LANES), size)
                    for n in range(8):
                        piece = y[n * rows : (n + 1) * rows, k * size : (k + 1) * size]
                        self.put(piece, n // 4, ranks[n % 4], cols)
        self.swap(self.group(self.x.at[0], q, i), self.group(self.x.at[1], q, i), self.sems["l"].at[q, i], other_core())

    def chip_sum(self, q, i):
        landed(self.group(self.x.at[1], q, i), self.sems["l"].at[q, i])
        cols = self.cols(2, i) if q == 2 else pl.ds(STARTS[q], SIZES[q])
        for at in self.ranks(q, i):
            own = self.s.at[(*at, slice(None), cols)]
            other = self.x[(1, *at, slice(None), slice(None), cols)]
            other = other.reshape(self.rows, other.shape[2])
            own[...] = (own[...].astype(jnp.float32) + other.astype(jnp.float32)).astype(jnp.bfloat16)

    def drain(self):
        width = self.s.shape[3]
        for send, part in zip(self.sends, (width, width // 4 * 3, width // 32 * 11)):
            send.drain(self.s.at[:, :, :, pl.ds(0, part)])

    def down(self, q, b):
        t = self.bufs[q][2]
        self.first[q].collect(b, t.at[b])

    def end(self, q, k):
        a, sems = ORDERS[q][2], self.sems
        u, f3, n3 = self.bufs[q][5:]
        self.second[q].collect(k, u.at[k])
        if k == 2:
            self.send(u.at[2], f3, sems["f3"].at[q], {a: shifted(a, 1)})
        elif k == 3:
            self.send(u.at[3], n3.at[1], sems["n3"].at[q], {a: shifted(a, -1)})
        elif k == 1:
            landed(f3, sems["f3"].at[q])
            add_up(u.at[1], [u.at[1], f3])
            self.send(u.at[1], n3.at[0], sems["n3"].at[q], {a: shifted(a, 1)})

    def piece(self, q, core, chip):
        return self.ob.at[core, :, pl.ds(pl.multiple_of(STARTS[q] + chip * QUARTERS[q], LANES), QUARTERS[q])]

    def share(self, q):
        c, xi = lax.axis_index("c"), lax.axis_index("x")
        u, _, n3 = self.bufs[q][5:]
        landed(n3, self.sems["n3"].at[q])
        done = self.piece(q, c, xi)
        add_up(done, [u.at[0], n3.at[0], n3.at[1]])
        for by in (2, 1, 3):
            self.send(done, done, self.sems["ox"].at[q, by - 1], {"x": shifted("x", by)})
        self.send(done, done, self.sems["od"].at[q], other_core())

    def pair(self, q, by):
        part = self.piece(q, lax.axis_index("c"), lax.rem(lax.axis_index("x") + 4 - by, 4))
        landed(part, self.sems["ox"].at[q, by - 1])
        self.send(part, part, self.sems["od"].at[q], other_core())

    def close(self, q):
        landed(self.ob.at[1 - lax.axis_index("c"), :, pl.ds(STARTS[q], SIZES[q])], self.sems["od"].at[q])


RECV = ("l", "f1", "n1", "f2", "n2", "f3", "n3", "ox", "od")


def moe_kernel(
    tok, ids, gates, live, wg_hbm, wu_hbm, wd_hbm, ob, loads, x, wg, wu, wd, m, wcol, hid, s, bufs,
    wsem, send_sem, meta_sem, free_sem, collect_sems, recv,
):
    weights = [
        pltpu.make_async_copy(src, dst, wsem.at[n])
        for n, (src, dst) in enumerate(((wg_hbm, wg), (wu_hbm, wu), (wd_hbm, wd)))
    ]
    for copy in weights:
        copy.start()
    count = tok.shape[0]
    token = lax.broadcasted_iota(jnp.int32, (8, count), 1)
    expert = lax.broadcasted_iota(jnp.int32, (8, count), 0)
    meta = jnp.zeros((8, count), jnp.float32)
    for k in range(2):
        named = (jnp.broadcast_to(ids[k : k + 1, :], (8, count)) == expert) & (token < live[0])
        meta = meta + jnp.where(named, jnp.broadcast_to(gates[k : k + 1, :], (8, count)), 0.0)
    m[0, 0] = meta
    enter([other_core(), {"x": shifted("x", 2)}] + [{a: shifted(a, by)} for a in ("x", "y", "z") for by in (1, -1)])
    send = Sender(send_sem.at[0, 0])
    gather, scatter = [], []
    per = tok.shape[0] // 2 // STREAMS
    for n in range(STREAMS):
        gather.append(
            Gather(
                Sender(send_sem.at[n, 1]), tok, x.at[n], n * per, [ref.at[n] for ref in collect_sems]
            )
        )
        sems = {name: ref.at[n] for name, ref in zip(RECV, recv)}
        parts = [tuple(buf.at[n] for buf in part) for part in bufs]
        scatter.append(Scatter(send_sem.at[n, pl.ds(2, 3)], hid.at[n], wd, x.at[n], s.at[n], ob.at[:, n], parts, sems))

    pass_meta(m, send, meta_sem, 0)
    relay = functools.partial(pass_meta, m, send, meta_sem)
    plan(gather, scatter, (wg, wu, wcol), hid, free_sem, weights, relay, lambda: weigh(m, meta_sem, wcol, loads))
    send.drain(wcol.at[0, pl.ds(0, 1), pl.ds(0, 120)])
    for each in scatter:
        each.drain()


ORDER = (
    2000, 1100, 3000, 3010, 1200, 5000, 5010, 4000, 5003, 6010, 6000, 8000, 5001, 4010,
    5011, 1300, 5013, 8010, 7000, 8003, 8001, 2100, 7010, 5002, 5012, 9000, 9010, 8011,
    0, 10000, 8012, 8013, 9003, 9001, 8002, 3110, 5110, 3100, 5100, 10010, 6110, 9002,
    9011, 9012, 9013, 10020, 10030, 6100, 4100, 5103, 5101, 8100, 8110, 4110, 5111, 5113,
    11000, 12022, 12012, 12021, 7100, 12002, 9110, 13022, 14020, 5102, 13012, 14010, 8103, 9100,
    13021, 15020, 12023, 7110, 8101, 13002, 14000, 5112, 12001, 8111, 12011, 10100, 9101, 8113,
    9103, 13001, 15000, 13023, 15021, 16020, 13011, 8102, 15010, 12020, 10110, 13020, 8112, 9113,
    12013, 9111, 16021, 12003, 17022, 18020, 10120, 17023, 17021, 19020, 17020, 9102, 9112, 20020,
    20021, 13003, 15001, 16000, 16001, 19021, 13013, 15011, 16010, 10130, 21022, 21023, 21020, 16011,
    11100, 12122, 12121, 12102, 12112, 12123, 21021, 13122, 14120, 13121, 15120, 12101, 13102, 14100,
    12111, 13112, 14110, 13123, 15121, 12120, 12113, 13101, 15100, 12103, 16120, 13120, 22020, 13111,
    15110, 13113, 15111, 16121, 12000, 13103, 15101, 16100, 12010, 12110, 16110, 13000, 17001, 19000,
    17002, 17003, 19001, 17000, 16101, 18000, 17121, 23023, 13110, 17122, 18120, 23021, 13010, 17012,
    17011, 17013, 19011, 19010, 17123, 18010, 23022, 17120, 19120, 12100, 24020, 19121, 17010, 16111,
    20000, 20001, 13100, 17102, 18100, 17101, 19100, 17112, 18110, 20120, 17100, 21002, 17111, 19110,
    21003, 21000, 20121, 17103, 19101, 20100, 20101, 17110, 20010, 21122, 20011, 21001, 17113, 19111,
    20110, 21120, 21102, 21123, 21012, 21121, 21103, 21010, 20111, 21112, 21101, 22000, 21013, 21100,
    21011, 22120, 21110, 21113, 21111, 22100, 23123, 23001, 23002, 23003, 22010, 23122, 24000, 23121,
    23103, 22110, 24120, 23102, 23101, 23013, 23012, 23011, 24100, 23113, 24010, 23111, 23112, 24110,
)
CHUNKS = (((0, 0), (0, 3), (0, 1), (0, 2)), ((3, 0), (1, 0), (3, 3), (1, 3)), ((3, 1), (1, 1), (3, 2), (1, 2)), ((2, 0), (2, 3), (2, 1), (2, 2)))


def plan(gather, scatter, weights_in, hid, free_sem, weights, relay, weigh_all):
    def compute(n, k):
        gather[n].compute(k, *weights_in, hid.at[n])

    def begin():
        for each in gather:
            each.fill()
        weigh_all()
        for copy in weights:
            copy.wait()

    def release(n):
        gather[n].send.drain(gather[n].x.at[:, :, :, :, :, pl.ds(0, gather[n].width // 32 * 30)])
        pl.semaphore_signal(free_sem.at[n], inc=1, device_id=other_core(), device_id_type=MESH)
        pl.semaphore_wait(free_sem.at[n], 1)

    steps = (
        (0, begin),
        (1, relay),
        (1, lambda n: gather[n].start()),
        (2, lambda n, h: gather[n].near(h)),
        (2, lambda n, h: gather[n].far(h)),
        (3, lambda n, h, b: gather[n].onward(h, b)),
        (2, lambda n, h: gather[n].joined_near(h)),
        (2, lambda n, h: gather[n].joined_far(h)),
        (3, lambda n, h, b: gather[n].joined(h, b)),
        (3, lambda n, h, b: gather[n].last(h, b)),
        (2, compute),
        (1, release),
        (3, lambda n, q, i: scatter[n].compute(q, i)),
        (3, lambda n, q, i: scatter[n].chip_sum(q, i)),
        (2, lambda n, q: scatter[n].first[q].send_far()),
        (3, lambda n, q, way: scatter[n].first[q].send_direct(way)),
        (3, lambda n, q, k: scatter[n].first[q].pass_on(k)),
        (3, lambda n, q, b: scatter[n].down(q, b)),
        (2, lambda n, q: scatter[n].second[q].send_far()),
        (3, lambda n, q, way: scatter[n].second[q].send_direct(way)),
        (3, lambda n, q, k: scatter[n].second[q].pass_on(k)),
        (3, lambda n, q, k: scatter[n].end(q, k)),
        (2, lambda n, q: scatter[n].share(q)),
        (3, lambda n, q, by: scatter[n].pair(q, by)),
        (2, lambda n, q: scatter[n].close(q)),
    )
    for code in ORDER:
        count, step = steps[code // 1000]
        step(*(code // place % 10 for place in (100, 10, 1)[:count]))


def per_device(tokens, expert_ids, gate_weights, live_counts, w_gate, w_up, w_down):
    count, width = tokens.shape
    depth = w_gate.shape[2]
    rows = count // 2 // STREAMS
    dma = pltpu.SemaphoreType.DMA
    bf16, f32 = jnp.bfloat16, jnp.float32
    vmem = pl.BlockSpec(memory_space=pltpu.VMEM)
    hbm = pl.BlockSpec(memory_space=pl.ANY)
    n = STREAMS
    bufs = []
    for q in range(3):
        wide = QUARTERS[q]
        one = (rows, 4 * wide) if q == 1 else (4, rows, wide)
        bufs.append(
            [
                pltpu.VMEM(shape, bf16)
                for shape in (
                    (n, 2, 2, *one), (n, 2, 4, *one), (n, 4, *one), (n, 2, 2, rows, wide), (n, 2, 4, rows, wide),
                    (n, 4, rows, wide), (n, rows, wide), (n, 2, rows, wide),
                )
            ]
        )
    mixed, loads = pl.pallas_call(
        moe_kernel,
        out_shape=(
            jax.ShapeDtypeStruct((2, n, rows, width), bf16),
            jax.ShapeDtypeStruct((1, 128), jnp.int32),
        ),
        in_specs=[vmem, vmem, vmem, pl.BlockSpec(memory_space=pltpu.SMEM), hbm, hbm, hbm],
        out_specs=(vmem, vmem),
        scratch_shapes=[
            pltpu.VMEM((n, 2, 4, 4, 2, rows // 2, width), bf16),
            pltpu.VMEM((width, depth), bf16),
            pltpu.VMEM((width, depth), bf16),
            pltpu.VMEM((depth, width), bf16),
            pltpu.VMEM((4, 4, 8, count), f32),
            pltpu.VMEM((4, 4, count, count), f32),
            pltpu.VMEM((n, 4, 4, 2, rows, depth), bf16),
            pltpu.VMEM((n, 4, 4, rows, width), bf16),
            bufs,
            dma((3,)),
            dma((n, 5)),
            dma((4,)),
            pltpu.SemaphoreType.REGULAR((n,)),
            [
                dma((n, 2)), dma((n, 2)), dma((n, 2, 4)), dma((n, 2, 2)), dma((n, 2, 4)), dma((n, 2, 4)),
                dma((n, len(CHUNKS))),
            ],
            [
                dma((n, 3, 4)), dma((n, 3, 2)), dma((n, 3, 4)), dma((n, 3, 2)), dma((n, 3, 4)),
                dma((n, 3)), dma((n, 3)), dma((n, 3, 3)), dma((n, 3)),
            ],
        ],
        compiler_params=pltpu.CompilerParams(
            collective_id=0, has_side_effects=True, vmem_limit_bytes=VMEM_LIMIT
        ),
        name="moe",
    )(tokens, expert_ids.T, gate_weights.T, live_counts, w_gate[0], w_up[0], w_down[0])
    return (mixed.reshape(count, width), loads[0, :8])


def solution(mesh):
    torus = Mesh(mesh.devices.reshape(4, 4, 4, 2), DP + EXPERT)
    in_specs = (
        P(DP, None),
        P(DP, None),
        P(DP, None),
        P(DP),
        P(EXPERT, None, DP),
        P(EXPERT, None, DP),
        P(EXPERT, DP, None),
    )
    out_specs = (P(DP, None), P())
    return jax.shard_map(
        per_device, mesh=torus, in_specs=in_specs, out_specs=out_specs, check_vma=False
    )
```
